32 devices in a mesh: aa: 4 (over z), ba: 8 (over y, x, core).
Axes of the slice: x: 2, y: 2, z: 4, core: 2. Of those that a mesh axis runs over, the one named last changes fastest.
Arguments:
- grad_out: bfloat16 [4096, 4096], P('aa', 'ba')
- saved_input: bfloat16 [4096, 4096], P(('aa', 'ba'))
- keep_bits: int32 [4096, 128], P(('aa', 'ba')), may hold values from -2147483648 to 2147483647, as said below
- gain: float32 [4096], replicated, may hold values from 0.5 to 1.5
Outputs:
- grad_in: bfloat16 [4096, 4096], P(('aa', 'ba'))
- gain_grad: float32 [4096], P('ba')
The draws below stay inside these ranges and needn't reach their ends.
Inputs may be any that keep to these rules, and one draw needn't show every extreme that they name: `keep_bits`: bit k of word w in row t (bit 31 being the sign bit) is the keep flag of feature 32 * w + k of token t; about nine in ten flags are 1.
All inputs are finite; a program needn't handle non-finite values.
Results may differ from the reference program's by a relative error of at most 0.001.
Values may be sent and summed in bfloat16 or wider, within the bound.
A program may use at most 64 MiB of HBM per device.

```python
import math
import jax
import jax.numpy as jnp
from jax import lax

D = 4096
TOKENS = 4096
WORDS = 128


def draw_grad_out(key, part):
    first = jax.random.fold_in(key, 11)
    second = jax.random.fold_in(key, 12)
    rise = 1.0 + 2.0 * jnp.arange(TOKENS, dtype=jnp.float32) / TOKENS
    rough = jnp.exp(jax.random.uniform(second, (TOKENS,), jnp.float32, jnp.log(0.5), jnp.log(2.0)))
    base = jax.random.normal(first, (TOKENS, D), jnp.float32)
    values = base * (rise * rough)[:, None]
    return values.astype(jnp.bfloat16)


def draw_saved_input(key, part):
    first = jax.random.fold_in(key, 21)
    second = jax.random.fold_in(key, 22)
    third = jax.random.fold_in(key, 23)
    base = jax.random.normal(first, (TOKENS, D), jnp.float32)
    row_scale = jnp.exp(jax.random.uniform(second, (TOKENS,), jnp.float32, jnp.log(0.3), jnp.log(3.0)))
    column_scale = jnp.exp(jax.random.uniform(third, (D,), jnp.float32, jnp.log(0.5), jnp.log(5.0)))
    values = base * row_scale[:, None] * column_scale[None, :]
    return values.astype(jnp.bfloat16)


def draw_keep_bits(key, part):
    picks = jax.random.randint(jax.random.fold_in(key, 31), (TOKENS, WORDS, 32), 0, 10)
    flags = (picks < 9).astype(jnp.int32)
    shifts = jnp.arange(32, dtype=jnp.int32)
    return jnp.sum(jnp.left_shift(flags, shifts[None, None, :]), axis=-1).astype(jnp.int32)


def setup_inputs(seed: int = 0) -> dict:
    seeds = jax.random.split(jax.random.key(seed), 5)
    grad_out = draw_grad_out(jax.random.fold_in(seeds[4], 71), 0)
    saved_input = draw_saved_input(jax.random.fold_in(seeds[4], 71), 0)
    keep_bits = draw_keep_bits(jax.random.fold_in(seeds[4], 71), 0)
    gain = jnp.clip(1.0 + 0.1 * jax.random.normal(seeds[3], (D,), jnp.float32), 0.5, 1.5)
    return {"grad_out": grad_out, "saved_input": saved_input, "keep_bits": keep_bits, "gain": gain}


KEEP_RATE = 0.9
EPSILON = 1e-06

def unpack_bits(words):
    shifts = jnp.arange(32, dtype=jnp.int32)
    bits = jnp.right_shift(words[:, :, None], shifts[None, None, :]) & 1
    return bits.reshape(words.shape[0], words.shape[1] * 32).astype(jnp.float32)

def rows_backward(grad_rows, input_rows, word_rows, gain):
    keep = unpack_bits(word_rows)
    dropped = input_rows.astype(jnp.float32) * keep * (1.0 / KEEP_RATE)
    inverse = lax.rsqrt(lax.optimization_barrier(jnp.mean(dropped * dropped, axis=-1, keepdims=True)) + EPSILON)
    normed = dropped * inverse
    grads = grad_rows.astype(jnp.float32)
    scaled = gain[None, :] * grads
    centre = lax.optimization_barrier(jnp.mean(scaled * normed, axis=-1, keepdims=True))
    grad_in = (inverse * (scaled - normed * centre) * keep * (1.0 / KEEP_RATE)).astype(jnp.bfloat16)
    partial_sum = lax.optimization_barrier(jnp.sum(grads * normed, axis=0))
    return (grad_in, partial_sum)

def reference(grad_out, saved_input, keep_bits, gain):
    block = math.gcd(TOKENS, 512)
    count = TOKENS // block

    def one_block(items):
        return rows_backward(items[0], items[1], items[2], gain)
    grad_in, partial_sums = lax.map(one_block, (grad_out.reshape(count, block, D), saved_input.reshape(count, block, D), keep_bits.reshape(count, block, WORDS)))
    gain_grad = lax.optimization_barrier(jnp.sum(partial_sums, axis=0)) * (1.0 / math.sqrt(TOKENS))
    return (grad_in.reshape(TOKENS, D), gain_grad)
```

```python
import functools
import math

import jax
import jax.numpy as jnp
from jax import lax
from jax.experimental import pallas as pl
from jax.experimental.pallas import tpu as pltpu
from jax.sharding import PartitionSpec as P

KEEP_RATE = 0.9
EPSILON = 1e-06
LANES = 128
CHUNK_ROWS = 64
STORES = 4
FIRST_ROWS = 32
EARLY_ROWS = 64
MESH = pl.DeviceIdType.MESH


def unpack_bits(words):
    shifts = jnp.arange(32, dtype=jnp.int32)
    bits = jnp.right_shift(words[:, :, None], shifts[None, None, :]) & 1
    return bits.reshape(words.shape[0], words.shape[1] * 32).astype(jnp.float32)


def rows_backward(grad_rows, input_rows, word_rows, gain):
    keep = unpack_bits(word_rows)
    dropped = input_rows.astype(jnp.float32) * keep * (1.0 / KEEP_RATE)
    inverse = lax.rsqrt(jnp.mean(dropped * dropped, axis=-1, keepdims=True) + EPSILON)
    normed = dropped * inverse
    grads = grad_rows.astype(jnp.float32)
    scaled = gain[None, :] * grads
    centre = jnp.mean(scaled * normed, axis=-1, keepdims=True)
    grad_in = (inverse * (scaled - normed * centre) * keep * (1.0 / KEEP_RATE)).astype(jnp.bfloat16)
    partial_sum = jnp.sum(grads * normed, axis=0)
    return (grad_in, partial_sum)


def plain(grad_out, saved_input, keep_bits, gain):
    groups = lax.axis_size("ba")
    rows = grad_out.shape[0] // groups
    pieces = grad_out.reshape(groups, rows, grad_out.shape[1])
    arrived = lax.all_to_all(pieces, "ba", split_axis=0, concat_axis=2, tiled=True)
    grad_rows = arrived.reshape(rows, arrived.shape[2])
    grad_in, partial_sum = rows_backward(grad_rows, saved_input, keep_bits, gain)
    total_tokens = rows * groups * lax.axis_size("aa")
    owned = lax.psum_scatter(partial_sum, "ba", scatter_dimension=0, tiled=True)
    share = lax.psum(owned, "aa")
    gain_grad = share * (1.0 / math.sqrt(total_tokens))
    return (grad_in, gain_grad)


def hops(step):
    return (step >> 1).bit_count()


def steps_with(n_ba, count):
    return sorted((step for step in range(n_ba) if hops(step) == count), key=lambda step: (step % 2, step))


def kernel(n_ba, n_aa, grad_hbm, input_hbm, bits_hbm, gain_hbm, out_ref, share_ref,
           staged, arrived, held, words, gain_ref, normed, masked_gain, outer, totals, sums,
           parts, slices, tails, stage_sem, load_sem, send_sem, small_send, early_recv,
           last_recv, diagonal_recv, sibling_recv, part_recv, tail_recv, ready, flood):
    ba, aa = lax.axis_index("ba"), lax.axis_index("aa")
    rows, width = arrived.shape[1], arrived.shape[2]
    depth = n_ba * width
    chunks = rows // CHUNK_ROWS
    tiles = width // LANES
    direct, diagonal = steps_with(n_ba, 1), steps_with(n_ba, 2)
    n_direct, n_diagonal = len(direct), len(diagonal)
    half = n_direct // 2
    group = n_direct + n_diagonal + 1
    order = [0, 1] + direct + diagonal
    slot = {step: place for place, step in enumerate(order)}
    swap = lax.rem(ba // (2 * direct[0]), 2)
    arrivals = [
        (side + offset, 2 + (half if side else 0) + index)
        for offset, index in ((2 + 2 * swap, swap), (4 - 2 * swap, 1 - swap))
        for side in range(2)
    ]
    early, last = (0, EARLY_ROWS), (EARLY_ROWS, rows - EARLY_ROWS)

    def remote_copy(source, target, send, recv, device):
        return pltpu.make_async_remote_copy(
            src_ref=source, dst_ref=target, send_sem=send, recv_sem=recv,
            device_id=device, device_id_type=MESH,
        )

    def column(step):
        return lax.rem(aa + step, n_aa)

    def rows_of(chunk):
        start = chunk * CHUNK_ROWS
        if not isinstance(start, int):
            start = pl.multiple_of(start, CHUNK_ROWS)
        return pl.ds(start, CHUNK_ROWS)

    def stage(step, semaphore):
        first = pl.ds(pl.multiple_of((ba ^ step) * rows, CHUNK_ROWS), rows)
        target = staged.at[slot[step]] if step else arrived.at[0]
        return pltpu.make_async_copy(grad_hbm.at[first], target, semaphore)

    def piece(step, recv, block=None, place=None):
        place = slot[step] if place is None else place
        at = (place, pl.ds(*block)) if block else (place,)
        return remote_copy(staged.at[at], arrived.at[at], send_sem, recv, {"ba": ba ^ step})

    def early_piece(step):
        return piece(step, early_recv, early)

    def last_piece(step, place):
        return piece(step, last_recv.at[place - 2], last, place)

    def landed(recv, *at):
        return remote_copy(staged.at[at], arrived.at[at], send_sem, recv, {"ba": ba ^ 1})

    def part():
        return remote_copy(parts.at[1], slices.at[1], small_send, part_recv, {"ba": ba ^ 1})

    def share(step):
        mine = tails.at[aa * group]
        return remote_copy(mine, mine, small_send, tail_recv, {"aa": column(step)})

    def late(target, step, place):
        return remote_copy(
            parts.at[place], tails.at[aa * group + place - 1], small_send, tail_recv,
            {"aa": target, "ba": ba ^ step},
        )

    def greet_column(semaphore):
        @pl.when(aa > 0)
        def _():
            pl.semaphore_signal(semaphore, inc=1, device_id={"aa": aa - 1}, device_id_type=MESH)

        @pl.when(aa < n_aa - 1)
        def _():
            pl.semaphore_signal(semaphore, inc=1, device_id={"aa": aa + 1}, device_id_type=MESH)

    column_peers = (aa > 0).astype(jnp.int32) + (aa < n_aa - 1).astype(jnp.int32)

    barrier = pltpu.get_barrier_semaphore()
    for step in direct + [1]:
        pl.semaphore_signal(barrier, inc=1, device_id={"ba": ba ^ step}, device_id_type=MESH)
    greet_column(barrier)
    for step in order[1:]:
        stage(step, stage_sem).start()
    loads = [
        pltpu.make_async_copy(bits_hbm, words, load_sem),
        pltpu.make_async_copy(gain_hbm, gain_ref, load_sem),
        pltpu.make_async_copy(input_hbm, held, load_sem),
        stage(0, load_sem),
    ]
    for load in loads:
        load.start()
    with jax.named_scope("w_barrier"):
        pl.semaphore_wait(barrier, n_direct + 1 + column_peers)
    pl.semaphore_signal(ready, inc=1, device_id={"ba": ba ^ direct[0]}, device_id_type=MESH)
    with jax.named_scope("w_stage"):
        everything = pl.ds(1, n_ba - 1)
        pltpu.make_async_copy(staged.at[everything], staged.at[everything], stage_sem).wait()
    for step in direct:
        early_piece(step).start()
    piece(1, sibling_recv).start()
    with jax.named_scope("w_ready"):
        pl.semaphore_wait(ready, 1)
    greet_column(flood.at[0])
    for step in diagonal:
        piece(step, diagonal_recv).start()
    for step in direct:
        last_piece(step, slot[step]).start()
    with jax.named_scope("w_load"):
        for load in loads:
            load.wait()

    lane = lax.broadcasted_iota(jnp.int32, (CHUNK_ROWS, LANES), 1)
    word_of = lane // 32
    flag = jnp.left_shift(jnp.int32(1), lane % 32)

    def span(source, tile):
        return pl.ds(pl.multiple_of(source * width + tile * LANES, LANES), LANES)

    def prepare(chunk, carry):
        block = rows_of(chunk)

        def drop(source, squares):
            row_words = words[block, :]
            for tile in range(tiles):
                at = span(source, tile)
                index = word_of + (source * tiles + tile) * (LANES // 32)
                spread = jnp.take_along_axis(row_words, index, axis=1, mode="promise_in_bounds")
                kept = (spread & flag) != 0
                dropped = jnp.where(kept, held[block, at].astype(jnp.float32), 0.0) * (1.0 / KEEP_RATE)
                normed[block, at] = dropped
                masked_gain[block, at] = jnp.where(kept, gain_ref[:, at], 0.0)
                squares = squares + dropped * dropped
            return squares

        squares = lax.fori_loop(0, n_ba, drop, jnp.zeros((CHUNK_ROWS, LANES), jnp.float32))
        mean = jnp.sum(squares, axis=1, keepdims=True) * (1.0 / depth)
        inverse = lax.rsqrt(mean + EPSILON)
        outer[block, :] = jnp.broadcast_to(inverse * (1.0 / KEEP_RATE), (CHUNK_ROWS, LANES))

        def scale(source, none):
            for tile in range(tiles):
                at = span(source, tile)
                normed[block, at] = normed[block, at] * inverse
            return none

        lax.fori_loop(0, n_ba, scale, 0)
        return carry

    with jax.named_scope("prepare"):
        lax.fori_loop(0, chunks, prepare, 0)
    sums[...] = jnp.zeros_like(sums)
    totals[...] = jnp.zeros_like(totals)

    def first(step, place, start, size):
        source = ba ^ step

        def some(index, none):
            block = pl.ds(pl.multiple_of(start + index * FIRST_ROWS, FIRST_ROWS), FIRST_ROWS)
            total = totals[block, :]
            for tile in range(tiles):
                at = span(source, tile)
                here = slice(tile * LANES, (tile + 1) * LANES)
                grads = arrived[place, block, here].astype(jnp.float32)
                product = grads * normed[block, at]
                total = total + product * gain_ref[:, at]
                sums[place, :, here] += jnp.sum(product.reshape(FIRST_ROWS // 8, 8, LANES), axis=0)
            totals[block, :] = total
            return none

        lax.fori_loop(0, size // FIRST_ROWS, some, 0)

    def finish(chunk, none):
        block = rows_of(chunk)
        factor = outer[block, :]
        centre = jnp.sum(totals[block, :], axis=1, keepdims=True) * (1.0 / depth)

        for step in order:
            for tile in range(tiles):
                at = span(ba ^ step, tile)
                grads = arrived[slot[step], block, tile * LANES:(tile + 1) * LANES].astype(jnp.float32)
                value = factor * (masked_gain[block, at] * grads - normed[block, at] * centre)
                out_ref[block, at] = value.astype(jnp.bfloat16)
        return none

    def fold(place):
        return jnp.sum(sums[place], axis=0, keepdims=True)

    def send_late(step, place):
        parts[place] = fold(place)
        for target in range(n_aa):
            late(target, step, place).start()

    def meet(turn):
        with jax.named_scope(f"w_flood{turn}"):
            pl.semaphore_wait(flood.at[turn], column_peers)
        if turn < n_aa - 2:
            greet_column(flood.at[turn + 1])

    first(0, 0, 0, rows)
    slices[0] = fold(0)
    with jax.named_scope("w_sibling"):
        piece(1, sibling_recv).wait_recv()
    first(1, 1, 0, rows)
    parts[1] = fold(1)
    part().start()
    meet(0)
    with jax.named_scope("w_early"):
        landed(early_recv, pl.ds(2, n_direct), pl.ds(*early)).wait_recv()
    for step in direct:
        first(step, slot[step], *early)
    for turn in range(1, n_aa - 1):
        meet(turn)
    with jax.named_scope("w_part"):
        part().wait_recv()
    tails[aa * group] = slices[0] + slices[1]
    for step in range(1, n_aa):
        share(step).start()
    with jax.named_scope("w_diag"):
        landed(diagonal_recv, pl.ds(2 + n_direct, n_diagonal)).wait_recv()
    for step in diagonal:
        first(step, slot[step], 0, rows)
        send_late(step, slot[step])
    for step, place in arrivals:
        with jax.named_scope("w_last"):
            last_piece(step, place).wait_recv()
        first(step, place, *last)
        send_late(step, place)
    with jax.named_scope("finish"):
        lax.fori_loop(0, chunks, finish, 0)
    with jax.named_scope("w_tail"):
        others = tails.at[pl.ds(0, n_aa * group - 1)]
        remote_copy(others, others, small_send, tail_recv, {"ba": ba ^ 1}).wait_recv()
    with jax.named_scope("final_sum"):
        total = jnp.sum(tails[...], axis=0)
        share_ref[...] = total * (1.0 / math.sqrt(rows * n_ba * n_aa))
    with jax.named_scope("w_last_sends"):
        landed(sibling_recv, everything).wait_send()
        remote_copy(tails, tails, small_send, tail_recv, {"ba": ba ^ 1}).wait_send()


def store(grad_vmem, share_vmem, grad_hbm, share_hbm, sem):
    rows = grad_vmem.shape[0] // STORES
    copies = [pltpu.make_async_copy(share_vmem, share_hbm, sem.at[1])]
    for index in range(STORES):
        block = pl.ds(index * rows, rows)
        copies.append(pltpu.make_async_copy(grad_vmem.at[block], grad_hbm.at[block], sem.at[0]))
    for copy in copies:
        copy.start()
    pltpu.make_async_copy(grad_vmem, grad_hbm, sem.at[0]).wait()
    copies[0].wait()


def fused(grad_out, saved_input, keep_bits, gain):
    n_ba, n_aa = lax.axis_size("ba"), lax.axis_size("aa")
    width = grad_out.shape[1]
    rows, depth = saved_input.shape
    n_direct, n_diagonal = len(steps_with(n_ba, 1)), len(steps_with(n_ba, 2))
    f32 = jnp.float32
    grad_in, share = pl.pallas_call(
        functools.partial(kernel, n_ba, n_aa),
        out_shape=(
            pltpu.VMEM((rows, depth), jnp.bfloat16),
            pltpu.VMEM((1, width), f32),
        ),
        in_specs=[pl.BlockSpec(memory_space=pl.ANY)] * 4,
        out_specs=(pl.BlockSpec(memory_space=pltpu.VMEM), pl.BlockSpec(memory_space=pltpu.VMEM)),
        scratch_shapes=[
            pltpu.VMEM((n_ba, rows, width), jnp.bfloat16),
            pltpu.VMEM((n_ba, rows, width), jnp.bfloat16),
            pltpu.VMEM((rows, depth), jnp.bfloat16),
            pltpu.VMEM(keep_bits.shape, jnp.int32),
            pltpu.VMEM((1, depth), f32),
            pltpu.VMEM((rows, depth), f32),
            pltpu.VMEM((rows, depth), f32),
            pltpu.VMEM((rows, LANES), f32),
            pltpu.VMEM((rows, LANES), f32),
            pltpu.VMEM((n_ba, 8, width), f32),
            pltpu.VMEM((n_ba, 1, width), f32),
            pltpu.VMEM((2, 1, width), f32),
            pltpu.VMEM((n_aa * (n_direct + n_diagonal + 1), 1, width), f32),
            pltpu.SemaphoreType.DMA,
            pltpu.SemaphoreType.DMA,
            pltpu.SemaphoreType.DMA,
            pltpu.SemaphoreType.DMA,
            pltpu.SemaphoreType.DMA,
            pltpu.SemaphoreType.DMA((n_direct,)),
            pltpu.SemaphoreType.DMA,
            pltpu.SemaphoreType.DMA,
            pltpu.SemaphoreType.DMA,
            pltpu.SemaphoreType.DMA,
            pltpu.SemaphoreType.REGULAR,
            pltpu.SemaphoreType.REGULAR((n_aa - 1,)),
        ],
        compiler_params=pltpu.CompilerParams(collective_id=0, has_side_effects=True),
        name="regroup_backward",
    )(grad_out, saved_input, keep_bits, gain.reshape(1, depth))
    grad_in, share = pl.pallas_call(
        store,
        out_shape=(
            jax.ShapeDtypeStruct((rows, depth), jnp.bfloat16),
            jax.ShapeDtypeStruct((1, width), f32),
        ),
        in_specs=[pl.BlockSpec(memory_space=pltpu.VMEM)] * 2,
        out_specs=[pl.BlockSpec(memory_space=pl.ANY)] * 2,
        scratch_shapes=[pltpu.SemaphoreType.DMA((2,))],
        name="store_results",
    )(*(pltpu.with_memory_space_constraint(x, pltpu.VMEM) for x in (grad_in, share)))
    return (grad_in, share.reshape(width))


def per_device(grad_out, saved_input, keep_bits, gain):
    fits = grad_out.shape[1] % LANES == 0 and saved_input.shape[0] % CHUNK_ROWS == 0
    fits = fits and keep_bits.shape[1] == LANES
    n_ba = lax.axis_size("ba")
    fits = fits and n_ba & (n_ba - 1) == 0 and hops(n_ba - 1) == 2 and lax.axis_size("aa") > 1
    body = fused if fits else plain
    return body(grad_out, saved_input, keep_bits, gain)


def solution(mesh):
    placed = (P("aa", "ba"), P(("aa", "ba"), None), P(("aa", "ba"), None), P())
    return jax.shard_map(
        per_device,
        mesh=mesh,
        in_specs=placed,
        out_specs=(P(("aa", "ba"), None), P("ba")),
        check_vma=False,
    )
```

```python
import functools
import math

import jax
import jax.numpy as jnp
from jax import lax
from jax.experimental import pallas as pl
from jax.experimental.pallas import tpu as pltpu
from jax.sharding import PartitionSpec as P

KEEP_RATE = 0.9
EPSILON = 1e-06
LANES = 128
CHUNK_ROWS = 64
STORES = 4
FIRST_ROWS = 64
EARLY_ROWS = 64
CORNER_ROWS = 16
MESH = pl.DeviceIdType.MESH


def unpack_bits(words):
    shifts = jnp.arange(32, dtype=jnp.int32)
    bits = jnp.right_shift(words[:, :, None], shifts[None, None, :]) & 1
    return bits.reshape(words.shape[0], words.shape[1] * 32).astype(jnp.float32)


def rows_backward(grad_rows, input_rows, word_rows, gain):
    keep = unpack_bits(word_rows)
    dropped = input_rows.astype(jnp.float32) * keep * (1.0 / KEEP_RATE)
    inverse = lax.rsqrt(jnp.mean(dropped * dropped, axis=-1, keepdims=True) + EPSILON)
    normed = dropped * inverse
    grads = grad_rows.astype(jnp.float32)
    scaled = gain[None, :] * grads
    centre = jnp.mean(scaled * normed, axis=-1, keepdims=True)
    grad_in = (inverse * (scaled - normed * centre) * keep * (1.0 / KEEP_RATE)).astype(jnp.bfloat16)
    partial_sum = jnp.sum(grads * normed, axis=0)
    return (grad_in, partial_sum)


def plain(grad_out, saved_input, keep_bits, gain):
    groups = lax.axis_size("ba")
    rows = grad_out.shape[0] // groups
    pieces = grad_out.reshape(groups, rows, grad_out.shape[1])
    arrived = lax.all_to_all(pieces, "ba", split_axis=0, concat_axis=2, tiled=True)
    grad_rows = arrived.reshape(rows, arrived.shape[2])
    grad_in, partial_sum = rows_backward(grad_rows, saved_input, keep_bits, gain)
    total_tokens = rows * groups * lax.axis_size("aa")
    owned = lax.psum_scatter(partial_sum, "ba", scatter_dimension=0, tiled=True)
    share = lax.psum(owned, "aa")
    gain_grad = share * (1.0 / math.sqrt(total_tokens))
    return (grad_in, gain_grad)


def hops(step):
    return (step >> 1).bit_count()


def steps_with(n_ba, count):
    return sorted((step for step in range(n_ba) if hops(step) == count), key=lambda step: (step % 2, step))


def kernel(n_ba, n_aa, grad_hbm, input_hbm, bits_hbm, gain_hbm, out_ref, share_ref,
           staged, arrived, held, words, gain_ref, normed, masked_gain, outer, totals, sums,
           parts, slices, tails, stage_sem, load_sem, send_sem, small_send, early_recv,
           last_recv, diagonal_recv, sibling_recv, part_recv, tail_recv, ready, flood,
           relayed, relay_recv, relay_send, corner_recv):
    ba, aa = lax.axis_index("ba"), lax.axis_index("aa")
    rows, width = arrived.shape[1], arrived.shape[2]
    depth = n_ba * width
    chunks = rows // CHUNK_ROWS
    tiles = width // LANES
    direct, diagonal = steps_with(n_ba, 1), steps_with(n_ba, 2)
    n_direct, n_diagonal = len(direct), len(diagonal)
    half = n_direct // 2
    group = n_direct + n_diagonal + 1
    order = [0, 1] + direct + diagonal
    slot = {step: place for place, step in enumerate(order)}
    swap = lax.rem(ba // (2 * direct[0]), 2)
    arrivals = [
        (side + offset, 2 + (half if side else 0) + index)
        for offset, index in ((2 + 2 * swap, swap), (4 - 2 * swap, 1 - swap))
        for side in range(2)
    ]
    early, last = (0, EARLY_ROWS), (EARLY_ROWS, rows - EARLY_ROWS)
    short, corner = (EARLY_ROWS, rows - EARLY_ROWS - CORNER_ROWS), (rows - CORNER_ROWS, CORNER_ROWS)
    pairs = n_aa // 2
    shift = n_aa - pairs
    side = lax.rem(ba, 2)
    upper = aa >= shift
    relays = jnp.logical_and(aa < pairs, side == 1)

    def remote_copy(source, target, send, recv, device):
        return pltpu.make_async_remote_copy(
            src_ref=source, dst_ref=target, send_sem=send, recv_sem=recv,
            device_id=device, device_id_type=MESH,
        )

    def column(step):
        return lax.rem(aa + step, n_aa)

    def rows_of(chunk):
        start = chunk * CHUNK_ROWS
        if not isinstance(start, int):
            start = pl.multiple_of(start, CHUNK_ROWS)
        return pl.ds(start, CHUNK_ROWS)

    def stage(step, semaphore):
        first = pl.ds(pl.multiple_of((ba ^ step) * rows, CHUNK_ROWS), rows)
        target = staged.at[slot[step]] if step else arrived.at[0]
        return pltpu.make_async_copy(grad_hbm.at[first], target, semaphore)

    def piece(step, recv, block=None, place=None):
        place = slot[step] if place is None else place
        at = (place, pl.ds(*block)) if block else (place,)
        return remote_copy(staged.at[at], arrived.at[at], send_sem, recv, {"ba": ba ^ step})

    def early_piece(step, place):
        return piece(step, early_recv.at[place - 2], early, place)

    def last_piece(step, place, block):
        return piece(step, last_recv.at[place - 2], block, place)

    def to_relay(step):
        target = ba ^ step
        parity = lax.rem(target, 2)
        return remote_copy(
            staged.at[slot[step], pl.ds(*corner)], relayed.at[parity, slot[step] - 2], send_sem, relay_recv,
            {"aa": aa - shift, "ba": target + 1 - parity},
        )

    def from_relay(parity, place):
        return remote_copy(
            relayed.at[parity, place], arrived.at[place + 2, pl.ds(*corner)], relay_send, corner_recv,
            {"aa": aa + shift, "ba": ba - 1 + parity},
        )

    def relay_all():
        return remote_copy(relayed, relayed, relay_send, relay_recv, {"ba": ba ^ 1})

    def landed(recv, *at):
        return remote_copy(staged.at[at], arrived.at[at], send_sem, recv, {"ba": ba ^ 1})

    def part():
        return remote_copy(parts.at[1], slices.at[1], small_send, part_recv, {"ba": ba ^ 1})

    def share(step):
        mine = tails.at[aa * group]
        return remote_copy(mine, mine, small_send, tail_recv, {"aa": column(step)})

    def late(target, step, place):
        return remote_copy(
            parts.at[place], tails.at[aa * group + place - 1], small_send, tail_recv,
            {"aa": target, "ba": ba ^ step},
        )

    def greet_column(semaphore):
        @pl.when(aa > 0)
        def _():
            pl.semaphore_signal(semaphore, inc=1, device_id={"aa": aa - 1}, device_id_type=MESH)

        @pl.when(aa < n_aa - 1)
        def _():
            pl.semaphore_signal(semaphore, inc=1, device_id={"aa": aa + 1}, device_id_type=MESH)

    column_peers = (aa > 0).astype(jnp.int32) + (aa < n_aa - 1).astype(jnp.int32)

    barrier = pltpu.get_barrier_semaphore()
    for step in direct + [1]:
        pl.semaphore_signal(barrier, inc=1, device_id={"ba": ba ^ step}, device_id_type=MESH)
    greet_column(barrier)

    @pl.when(relays)
    def _():
        for step in direct:
            pl.semaphore_signal(
                barrier, inc=1, device_id={"aa": aa + shift, "ba": ba ^ step}, device_id_type=MESH)

    for step in order[1:]:
        stage(step, stage_sem).start()
    loads = [
        pltpu.make_async_copy(bits_hbm, words, load_sem),
        pltpu.make_async_copy(gain_hbm, gain_ref, load_sem),
        pltpu.make_async_copy(input_hbm, held, load_sem),
        stage(0, load_sem),
    ]
    for load in loads:
        load.start()
    with jax.named_scope("w_barrier"):
        pl.semaphore_wait(barrier, n_direct + 1 + column_peers + half * upper.astype(jnp.int32))
    pl.semaphore_signal(ready, inc=1, device_id={"ba": ba ^ direct[0]}, device_id_type=MESH)
    with jax.named_scope("w_stage"):
        everything = pl.ds(1, n_ba - 1)
        pltpu.make_async_copy(staged.at[everything], staged.at[everything], stage_sem).wait()
    for step in direct:
        early_piece(step, slot[step]).start()
    @pl.when(upper)
    def _():
        for step in direct:
            to_relay(step).start()

    piece(1, sibling_recv).start()
    with jax.named_scope("w_ready"):
        pl.semaphore_wait(ready, 1)
    greet_column(flood.at[0])
    for step in diagonal:
        piece(step, diagonal_recv).start()

    @pl.when(upper)
    def _():
        for step in direct:
            last_piece(step, slot[step], short).start()

    @pl.when(jnp.logical_not(upper))
    def _():
        for step in direct:
            last_piece(step, slot[step], last).start()

    with jax.named_scope("w_load"):
        for load in loads:
            load.wait()

    lane = lax.broadcasted_iota(jnp.int32, (CHUNK_ROWS, LANES), 1)
    word_of = lane // 32
    flag = jnp.left_shift(jnp.int32(1), lane % 32)

    def span(source, tile):
        return pl.ds(pl.multiple_of(source * width + tile * LANES, LANES), LANES)

    def prepare(chunk, carry):
        block = rows_of(chunk)

        def drop(source, squares):
            row_words = words[block, :]
            for tile in range(tiles):
                at = span(source, tile)
                index = word_of + (source * tiles + tile) * (LANES // 32)
                spread = jnp.take_along_axis(row_words, index, axis=1, mode="promise_in_bounds")
                kept = (spread & flag) != 0
                dropped = jnp.where(kept, held[block, at].astype(jnp.float32), 0.0) * (1.0 / KEEP_RATE)
                normed[block, at] = dropped
                masked_gain[block, at] = jnp.where(kept, gain_ref[:, at], 0.0)
                squares = squares + dropped * dropped
            return squares

        squares = lax.fori_loop(0, n_ba, drop, jnp.zeros((CHUNK_ROWS, LANES), jnp.float32))
        mean = jnp.sum(squares, axis=1, keepdims=True) * (1.0 / depth)
        inverse = lax.rsqrt(mean + EPSILON)
        outer[block, :] = jnp.broadcast_to(inverse * (1.0 / KEEP_RATE), (CHUNK_ROWS, LANES))

        def scale(source, none):
            for tile in range(tiles):
                at = span(source, tile)
                normed[block, at] = normed[block, at] * inverse
            return none

        lax.fori_loop(0, n_ba, scale, 0)
        return carry

    with jax.named_scope("prepare"):
        lax.fori_loop(0, chunks, prepare, 0)
    sums[...] = jnp.zeros_like(sums)
    totals[...] = jnp.zeros_like(totals)

    def first(step, place, start, size):
        source, count = ba ^ step, math.gcd(start, size, FIRST_ROWS)

        def some(index, none):
            block = pl.ds(pl.multiple_of(start + index * count, count), count)
            total = totals[block, :]
            for tile in range(tiles):
                at = span(source, tile)
                here = slice(tile * LANES, (tile + 1) * LANES)
                grads = arrived[place, block, here].astype(jnp.float32)
                product = grads * normed[block, at]
                total = total + product * gain_ref[:, at]
                sums[place, :, here] += jnp.sum(product.reshape(count // 8, 8, LANES), axis=0)
            totals[block, :] = total
            return none

        lax.fori_loop(0, size // count, some, 0)

    def finish(chunk, none):
        block = rows_of(chunk)
        factor = outer[block, :]
        centre = jnp.sum(totals[block, :], axis=1, keepdims=True) * (1.0 / depth)

        for step in order:
            for tile in range(tiles):
                at = span(ba ^ step, tile)
                grads = arrived[slot[step], block, tile * LANES:(tile + 1) * LANES].astype(jnp.float32)
                value = factor * (masked_gain[block, at] * grads - normed[block, at] * centre)
                out_ref[block, at] = value.astype(jnp.bfloat16)
        return none

    def fold(place):
        return jnp.sum(sums[place], axis=0, keepdims=True)

    def send_late(step, place):
        parts[place] = fold(place)
        for target in range(n_aa):
            late(target, step, place).start()

    def meet(turn):
        with jax.named_scope(f"w_flood{turn}"):
            pl.semaphore_wait(flood.at[turn], column_peers)
        if turn < n_aa - 2:
            greet_column(flood.at[turn + 1])

    def take_early(steps):
        for step, place in steps:
            with jax.named_scope("w_early"):
                early_piece(step, place).wait_recv()
            first(step, place, *early)

    first(0, 0, 0, rows)
    slices[0] = fold(0)
    with jax.named_scope("w_sibling"):
        piece(1, sibling_recv).wait_recv()
    first(1, 1, 0, rows)
    parts[1] = fold(1)
    part().start()
    meet(0)

    @pl.when(relays)
    def _():
        with jax.named_scope("w_relay"):
            relay_all().wait_recv()
        for parity in range(2):
            for place in range(n_direct):
                from_relay(parity, place).start()

    for turn in range(1, n_aa - 1):
        meet(turn)
    with jax.named_scope("w_part"):
        part().wait_recv()
    tails[aa * group] = slices[0] + slices[1]
    for step in range(1, n_aa):
        share(step).start()
    take_early(arrivals[:half])
    with jax.named_scope("w_diag"):
        landed(diagonal_recv, pl.ds(2 + n_direct, n_diagonal)).wait_recv()
    for step in diagonal:
        first(step, slot[step], 0, rows)
        send_late(step, slot[step])

    @pl.when(upper)
    def _():
        with jax.named_scope("w_corner"):
            landed(corner_recv, pl.ds(2, n_direct), pl.ds(*corner)).wait_recv()
        for step in direct:
            first(step, slot[step], *corner)

    for stage_index, some_arrivals in enumerate((arrivals[:half], arrivals[half:])):
        if stage_index:
            take_early(some_arrivals)
        for step, place in some_arrivals:
            @pl.when(upper)
            def _(step=step, place=place):
                with jax.named_scope("w_last"):
                    last_piece(step, place, short).wait_recv()
                first(step, place, *short)

            @pl.when(jnp.logical_not(upper))
            def _(step=step, place=place):
                with jax.named_scope("w_last"):
                    last_piece(step, place, last).wait_recv()
                first(step, place, *last)

            send_late(step, place)
    with jax.named_scope("finish"):
        lax.fori_loop(0, chunks, finish, 0)
    with jax.named_scope("w_tail"):
        others = tails.at[pl.ds(0, n_aa * group - 1)]
        remote_copy(others, others, small_send, tail_recv, {"ba": ba ^ 1}).wait_recv()
    with jax.named_scope("final_sum"):
        total = jnp.sum(tails[...], axis=0)
        share_ref[...] = total * (1.0 / math.sqrt(rows * n_ba * n_aa))
    with jax.named_scope("w_last_sends"):
        landed(sibling_recv, everything).wait_send()

        @pl.when(relays)
        def _():
            relay_all().wait_send()

        remote_copy(tails, tails, small_send, tail_recv, {"ba": ba ^ 1}).wait_send()


def store(grad_vmem, share_vmem, grad_hbm, share_hbm, sem):
    rows = grad_vmem.shape[0] // STORES
    copies = [pltpu.make_async_copy(share_vmem, share_hbm, sem.at[1])]
    for index in range(STORES):
        block = pl.ds(index * rows, rows)
        copies.append(pltpu.make_async_copy(grad_vmem.at[block], grad_hbm.at[block], sem.at[0]))
    for copy in copies:
        copy.start()
    pltpu.make_async_copy(grad_vmem, grad_hbm, sem.at[0]).wait()
    copies[0].wait()


def fused(grad_out, saved_input, keep_bits, gain):
    n_ba, n_aa = lax.axis_size("ba"), lax.axis_size("aa")
    width = grad_out.shape[1]
    rows, depth = saved_input.shape
    n_direct, n_diagonal = len(steps_with(n_ba, 1)), len(steps_with(n_ba, 2))
    f32 = jnp.float32
    grad_in, share = pl.pallas_call(
        functools.partial(kernel, n_ba, n_aa),
        out_shape=(
            pltpu.VMEM((rows, depth), jnp.bfloat16),
            pltpu.VMEM((1, width), f32),
        ),
        in_specs=[pl.BlockSpec(memory_space=pl.ANY)] * 4,
        out_specs=(pl.BlockSpec(memory_space=pltpu.VMEM), pl.BlockSpec(memory_space=pltpu.VMEM)),
        scratch_shapes=[
            pltpu.VMEM((n_ba, rows, width), jnp.bfloat16),
            pltpu.VMEM((n_ba, rows, width), jnp.bfloat16),
            pltpu.VMEM((rows, depth), jnp.bfloat16),
            pltpu.VMEM(keep_bits.shape, jnp.int32),
            pltpu.VMEM((1, depth), f32),
            pltpu.VMEM((rows, depth), f32),
            pltpu.VMEM((rows, depth), f32),
            pltpu.VMEM((rows, LANES), f32),
            pltpu.VMEM((rows, LANES), f32),
            pltpu.VMEM((n_ba, 8, width), f32),
            pltpu.VMEM((n_ba, 1, width), f32),
            pltpu.VMEM((2, 1, width), f32),
            pltpu.VMEM((n_aa * (n_direct + n_diagonal + 1), 1, width), f32),
            pltpu.SemaphoreType.DMA,
            pltpu.SemaphoreType.DMA,
            pltpu.SemaphoreType.DMA,
            pltpu.SemaphoreType.DMA,
            pltpu.SemaphoreType.DMA((n_direct,)),
            pltpu.SemaphoreType.DMA((n_direct,)),
            pltpu.SemaphoreType.DMA,
            pltpu.SemaphoreType.DMA,
            pltpu.SemaphoreType.DMA,
            pltpu.SemaphoreType.DMA,
            pltpu.SemaphoreType.REGULAR,
            pltpu.SemaphoreType.REGULAR((n_aa - 1,)),
            pltpu.VMEM((2, n_direct, CORNER_ROWS, width), jnp.bfloat16),
            pltpu.SemaphoreType.DMA,
            pltpu.SemaphoreType.DMA,
            pltpu.SemaphoreType.DMA,
        ],
        compiler_params=pltpu.CompilerParams(collective_id=0, has_side_effects=True),
        name="regroup_backward",
    )(grad_out, saved_input, keep_bits, gain.reshape(1, depth))
    grad_in, share = pl.pallas_call(
        store,
        out_shape=(
            jax.ShapeDtypeStruct((rows, depth), jnp.bfloat16),
            jax.ShapeDtypeStruct((1, width), f32),
        ),
        in_specs=[pl.BlockSpec(memory_space=pltpu.VMEM)] * 2,
        out_specs=[pl.BlockSpec(memory_space=pl.ANY)] * 2,
        scratch_shapes=[pltpu.SemaphoreType.DMA((2,))],
        name="store_results",
    )(*(pltpu.with_memory_space_constraint(x, pltpu.VMEM) for x in (grad_in, share)))
    return (grad_in, share.reshape(width))


def per_device(grad_out, saved_input, keep_bits, gain):
    fits = grad_out.shape[1] % LANES == 0 and saved_input.shape[0] % CHUNK_ROWS == 0
    fits = fits and keep_bits.shape[1] == LANES
    n_ba = lax.axis_size("ba")
    fits = fits and n_ba & (n_ba - 1) == 0 and hops(n_ba - 1) == 2 and lax.axis_size("aa") > 1
    body = fused if fits else plain
    return body(grad_out, saved_input, keep_bits, gain)


def solution(mesh):
    placed = (P("aa", "ba"), P(("aa", "ba"), None), P(("aa", "ba"), None), P())
    return jax.shard_map(
        per_device,
        mesh=mesh,
        in_specs=placed,
        out_specs=(P(("aa", "ba"), None), P("ba")),
        check_vma=False,
    )
```

```python
import functools
import math

import jax
import jax.numpy as jnp
from jax import lax
from jax.experimental import pallas as pl
from jax.experimental.pallas import tpu as pltpu
from jax.sharding import PartitionSpec as P

KEEP_RATE = 0.9
EPSILON = 1e-06
LANES = 128
CHUNK_ROWS = 64
STORES = 4
FIRST_ROWS = 64
EARLY_ROWS = 64
RELAY_ROWS = 16
MESH = pl.DeviceIdType.MESH


def unpack_bits(words):
    shifts = jnp.arange(32, dtype=jnp.int32)
    bits = jnp.right_shift(words[:, :, None], shifts[None, None, :]) & 1
    return bits.reshape(words.shape[0], words.shape[1] * 32).astype(jnp.float32)


def rows_backward(grad_rows, input_rows, word_rows, gain):
    keep = unpack_bits(word_rows)
    dropped = input_rows.astype(jnp.float32) * keep * (1.0 / KEEP_RATE)
    inverse = lax.rsqrt(jnp.mean(dropped * dropped, axis=-1, keepdims=True) + EPSILON)
    normed = dropped * inverse
    grads = grad_rows.astype(jnp.float32)
    scaled = gain[None, :] * grads
    centre = jnp.mean(scaled * normed, axis=-1, keepdims=True)
    grad_in = (inverse * (scaled - normed * centre) * keep * (1.0 / KEEP_RATE)).astype(jnp.bfloat16)
    partial_sum = jnp.sum(grads * normed, axis=0)
    return (grad_in, partial_sum)


def plain(grad_out, saved_input, keep_bits, gain):
    groups = lax.axis_size("ba")
    rows = grad_out.shape[0] // groups
    pieces = grad_out.reshape(groups, rows, grad_out.shape[1])
    arrived = lax.all_to_all(pieces, "ba", split_axis=0, concat_axis=2, tiled=True)
    grad_rows = arrived.reshape(rows, arrived.shape[2])
    grad_in, partial_sum = rows_backward(grad_rows, saved_input, keep_bits, gain)
    total_tokens = rows * groups * lax.axis_size("aa")
    owned = lax.psum_scatter(partial_sum, "ba", scatter_dimension=0, tiled=True)
    share = lax.psum(owned, "aa")
    gain_grad = share * (1.0 / math.sqrt(total_tokens))
    return (grad_in, gain_grad)


def hops(step):
    return (step >> 1).bit_count()


def steps_with(n_ba, count):
    return sorted((step for step in range(n_ba) if hops(step) == count), key=lambda step: (step % 2, step))


def kernel(n_ba, n_aa, grad_hbm, input_hbm, bits_hbm, gain_hbm, out_ref, share_ref,
           staged, arrived, held, words, gain_ref, normed, masked_gain, outer, totals, sums,
           parts, slices, tails, stage_sem, load_sem, send_sem, small_send, early_recv,
           last_recv, diagonal_recv, sibling_recv, part_recv, tail_recv, ready, flood,
           relayed, relay_recv, relay_send, corner_recv):
    ba, aa = lax.axis_index("ba"), lax.axis_index("aa")
    rows, width = arrived.shape[1], arrived.shape[2]
    depth = n_ba * width
    chunks = rows // CHUNK_ROWS
    tiles = width // LANES
    direct, diagonal = steps_with(n_ba, 1), steps_with(n_ba, 2)
    n_direct, n_diagonal = len(direct), len(diagonal)
    half = n_direct // 2
    per_plane = n_direct + n_diagonal + 1
    order = [0, 1] + direct + diagonal
    slot = {step: place for place, step in enumerate(order)}
    swap = lax.rem(ba // (2 * direct[0]), 2)
    arrivals = [
        (side + offset, 2 + (half if side else 0) + index)
        for offset, index in ((2 + 2 * swap, swap), (4 - 2 * swap, 1 - swap))
        for side in range(2)
    ]
    groups = (arrivals[:half], arrivals[half:])
    early = (0, EARLY_ROWS)
    first_chip = ba < 2
    beside = (ba ^ groups[0][0][0]) < 2
    never = ba < 0

    def amounts(plane, near_first):
        top = plane == n_aa - 1
        second = plane == n_aa - 2 if n_aa > 3 else never
        both = jnp.logical_and
        one = jnp.logical_or(both(top, jnp.logical_not(near_first)), both(second, near_first))
        return {1: one, 2: both(top, near_first)}

    mirror = n_aa - 1 - aa
    odd = lax.rem(ba, 2) == 1
    sends = amounts(aa, first_chip)
    fed = (amounts(aa, beside), amounts(aa, never))
    relays = tuple(
        {count: jnp.logical_and(flag, odd) for count, flag in amounts(mirror, near).items()}
        for near in (beside, never)
    )

    def either(flags):
        return jnp.logical_or(flags[1], flags[2])

    def last(count):
        return (EARLY_ROWS, rows - EARLY_ROWS - count * RELAY_ROWS)

    def relay_block(index, count=1):
        return pl.ds(rows - (index + count) * RELAY_ROWS, count * RELAY_ROWS)

    def for_count(flags, action):
        for count, flag in flags.items():
            pl.when(flag)(functools.partial(action, count))
        pl.when(jnp.logical_not(either(flags)))(functools.partial(action, 0))

    def remote_copy(source, target, send, recv, device):
        return pltpu.make_async_remote_copy(
            src_ref=source, dst_ref=target, send_sem=send, recv_sem=recv,
            device_id=device, device_id_type=MESH,
        )

    def column(step):
        return lax.rem(aa + step, n_aa)

    def rows_of(chunk):
        start = chunk * CHUNK_ROWS
        if not isinstance(start, int):
            start = pl.multiple_of(start, CHUNK_ROWS)
        return pl.ds(start, CHUNK_ROWS)

    def stage(step, semaphore):
        first = pl.ds(pl.multiple_of((ba ^ step) * rows, CHUNK_ROWS), rows)
        target = staged.at[slot[step]] if step else arrived.at[0]
        return pltpu.make_async_copy(grad_hbm.at[first], target, semaphore)

    def piece(step, recv, block=None, place=None):
        place = slot[step] if place is None else place
        at = (place, pl.ds(*block)) if block else (place,)
        return remote_copy(staged.at[at], arrived.at[at], send_sem, recv, {"ba": ba ^ step})

    def early_piece(step, place):
        return piece(step, early_recv.at[place - 2], early, place)

    def last_piece(step, place, block):
        return piece(step, last_recv.at[place - 2], block, place)

    def to_relay(step, index):
        target = ba ^ step
        parity = lax.rem(target, 2)
        swapped = lax.rem(target // (2 * direct[0]), 2)
        group = 1 - swapped if step >= 2 * direct[0] else swapped
        return remote_copy(
            staged.at[slot[step], relay_block(index)], relayed.at[group, index, parity, step % 2],
            send_sem, relay_recv.at[group], {"aa": mirror, "ba": target + 1 - parity},
        )

    def from_relay(group, index, parity, cross):
        return remote_copy(
            relayed.at[group, index, parity, cross], arrived.at[groups[group][cross][1], relay_block(index)],
            relay_send.at[group], corner_recv.at[group], {"aa": mirror, "ba": ba - 1 + parity},
        )

    def relay_all(group, count):
        blocks = relayed.at[group, pl.ds(0, count)]
        return remote_copy(blocks, blocks, relay_send.at[group], relay_recv.at[group], {"ba": ba ^ 1})

    def landed(recv, *at):
        return remote_copy(staged.at[at], arrived.at[at], send_sem, recv, {"ba": ba ^ 1})

    def part():
        return remote_copy(parts.at[1], slices.at[1], small_send, part_recv, {"ba": ba ^ 1})

    def share(step):
        mine = tails.at[aa * per_plane]
        return remote_copy(mine, mine, small_send, tail_recv, {"aa": column(step)})

    def late(target, step, place):
        return remote_copy(
            parts.at[place], tails.at[aa * per_plane + place - 1], small_send, tail_recv,
            {"aa": target, "ba": ba ^ step},
        )

    def greet_column(semaphore):
        @pl.when(aa > 0)
        def _():
            pl.semaphore_signal(semaphore, inc=1, device_id={"aa": aa - 1}, device_id_type=MESH)

        @pl.when(aa < n_aa - 1)
        def _():
            pl.semaphore_signal(semaphore, inc=1, device_id={"aa": aa + 1}, device_id_type=MESH)

    column_peers = (aa > 0).astype(jnp.int32) + (aa < n_aa - 1).astype(jnp.int32)

    barrier = pltpu.get_barrier_semaphore()
    for step in direct + [1]:
        pl.semaphore_signal(barrier, inc=1, device_id={"ba": ba ^ step}, device_id_type=MESH)
    greet_column(barrier)

    for group in range(2):
        @pl.when(either(relays[group]))
        def _(group=group):
            for step, _ in groups[group]:
                pl.semaphore_signal(
                    barrier, inc=1, device_id={"aa": mirror, "ba": ba ^ step}, device_id_type=MESH)

    for step in order[1:]:
        stage(step, stage_sem).start()
    loads = [
        pltpu.make_async_copy(bits_hbm, words, load_sem),
        pltpu.make_async_copy(gain_hbm, gain_ref, load_sem),
        pltpu.make_async_copy(input_hbm, held, load_sem),
        stage(0, load_sem),
    ]
    for load in loads:
        load.start()
    with jax.named_scope("w_barrier"):
        pl.semaphore_wait(barrier, n_direct + 1 + column_peers + half * either(sends).astype(jnp.int32))
    pl.semaphore_signal(ready, inc=1, device_id={"ba": ba ^ direct[0]}, device_id_type=MESH)
    with jax.named_scope("w_stage"):
        everything = pl.ds(1, n_ba - 1)
        pltpu.make_async_copy(staged.at[everything], staged.at[everything], stage_sem).wait()
    for step in direct:
        early_piece(step, slot[step]).start()

    @pl.when(either(sends))
    def _():
        for step in direct:
            to_relay(step, 0).start()

    @pl.when(sends[2])
    def _():
        for step in direct:
            to_relay(step, 1).start()

    piece(1, sibling_recv).start()
    with jax.named_scope("w_ready"):
        pl.semaphore_wait(ready, 1)
    greet_column(flood.at[0])
    for step in diagonal:
        piece(step, diagonal_recv).start()

    def start_last(count):
        for step in direct:
            last_piece(step, slot[step], last(count)).start()

    for_count(sends, start_last)
    with jax.named_scope("w_load"):
        for load in loads:
            load.wait()

    lane = lax.broadcasted_iota(jnp.int32, (CHUNK_ROWS, LANES), 1)
    word_of = lane // 32
    flag = jnp.left_shift(jnp.int32(1), lane % 32)

    def span(source, tile):
        return pl.ds(pl.multiple_of(source * width + tile * LANES, LANES), LANES)

    def prepare(chunk, carry):
        block = rows_of(chunk)

        def drop(source, squares):
            row_words = words[block, :]
            for tile in range(tiles):
                at = span(source, tile)
                index = word_of + (source * tiles + tile) * (LANES // 32)
                spread = jnp.take_along_axis(row_words, index, axis=1, mode="promise_in_bounds")
                kept = (spread & flag) != 0
                dropped = jnp.where(kept, held[block, at].astype(jnp.float32), 0.0) * (1.0 / KEEP_RATE)
                normed[block, at] = dropped
                masked_gain[block, at] = jnp.where(kept, gain_ref[:, at], 0.0)
                squares = squares + dropped * dropped
            return squares

        squares = lax.fori_loop(0, n_ba, drop, jnp.zeros((CHUNK_ROWS, LANES), jnp.float32))
        mean = jnp.sum(squares, axis=1, keepdims=True) * (1.0 / depth)
        inverse = lax.rsqrt(mean + EPSILON)
        outer[block, :] = jnp.broadcast_to(inverse * (1.0 / KEEP_RATE), (CHUNK_ROWS, LANES))

        def scale(source, none):
            for tile in range(tiles):
                at = span(source, tile)
                normed[block, at] = normed[block, at] * inverse
            return none

        lax.fori_loop(0, n_ba, scale, 0)
        return carry

    with jax.named_scope("prepare"):
        lax.fori_loop(0, chunks, prepare, 0)
    sums[...] = jnp.zeros_like(sums)
    totals[...] = jnp.zeros_like(totals)

    def first(step, place, start, size):
        source, count = ba ^ step, math.gcd(start, size, FIRST_ROWS)

        def some(index, none):
            block = pl.ds(pl.multiple_of(start + index * count, count), count)
            total = totals[block, :]
            for tile in range(tiles):
                at = span(source, tile)
                here = slice(tile * LANES, (tile + 1) * LANES)
                grads = arrived[place, block, here].astype(jnp.float32)
                product = grads * normed[block, at]
                total = total + product * gain_ref[:, at]
                sums[place, :, here] += jnp.sum(product.reshape(count // 8, 8, LANES), axis=0)
            totals[block, :] = total
            return none

        lax.fori_loop(0, size // count, some, 0)

    def finish(chunk, none):
        block = rows_of(chunk)
        factor = outer[block, :]
        centre = jnp.sum(totals[block, :], axis=1, keepdims=True) * (1.0 / depth)

        for step in order:
            for tile in range(tiles):
                at = span(ba ^ step, tile)
                grads = arrived[slot[step], block, tile * LANES:(tile + 1) * LANES].astype(jnp.float32)
                value = factor * (masked_gain[block, at] * grads - normed[block, at] * centre)
                out_ref[block, at] = value.astype(jnp.bfloat16)
        return none

    def fold(place):
        return jnp.sum(sums[place], axis=0, keepdims=True)

    def send_late(step, place):
        parts[place] = fold(place)
        for target in range(n_aa):
            late(target, step, place).start()

    def meet(turn):
        with jax.named_scope(f"w_flood{turn}"):
            pl.semaphore_wait(flood.at[turn], column_peers)
        if turn < n_aa - 2:
            greet_column(flood.at[turn + 1])

    def take_early(steps):
        for step, place in steps:
            with jax.named_scope("w_early"):
                early_piece(step, place).wait_recv()
            first(step, place, *early)

    first(0, 0, 0, rows)
    slices[0] = fold(0)
    with jax.named_scope("w_sibling"):
        piece(1, sibling_recv).wait_recv()
    first(1, 1, 0, rows)
    parts[1] = fold(1)
    part().start()
    meet(0)

    def pass_on(group, count):
        if count:
            with jax.named_scope("w_relay"):
                relay_all(group, count).wait_recv()
            for index in range(count):
                for parity in range(2):
                    for cross in range(2):
                        from_relay(group, index, parity, cross).start()

    for group in range(2):
        for_count(relays[group], functools.partial(pass_on, group))
    for turn in range(1, n_aa - 1):
        meet(turn)
    with jax.named_scope("w_part"):
        part().wait_recv()
    tails[aa * per_plane] = slices[0] + slices[1]
    for step in range(1, n_aa):
        share(step).start()
    def take_diagonal():
        with jax.named_scope("w_diag"):
            landed(diagonal_recv, pl.ds(2 + n_direct, n_diagonal)).wait_recv()
        for step in diagonal:
            first(step, slot[step], 0, rows)
            send_late(step, slot[step])

    def take_group(group, count):
        if count:
            with jax.named_scope("w_corner"):
                landed(corner_recv.at[group], pl.ds(2, half), relay_block(0, count)).wait_recv()
            for step, place in groups[group]:
                first(step, place, rows - count * RELAY_ROWS, count * RELAY_ROWS)
        for step, place in groups[group]:
            with jax.named_scope("w_last"):
                last_piece(step, place, last(count)).wait_recv()
            first(step, place, *last(count))
            send_late(step, place)

    take_early(groups[0])
    pl.when(jnp.logical_not(beside))(take_diagonal)
    for_count(fed[0], functools.partial(take_group, 0))
    pl.when(beside)(take_diagonal)
    take_early(groups[1])
    for_count(fed[1], functools.partial(take_group, 1))
    with jax.named_scope("finish"):
        lax.fori_loop(0, chunks, finish, 0)
    with jax.named_scope("w_tail"):
        others = tails.at[pl.ds(0, n_aa * per_plane - 1)]
        remote_copy(others, others, small_send, tail_recv, {"ba": ba ^ 1}).wait_recv()
    with jax.named_scope("final_sum"):
        total = jnp.sum(tails[...], axis=0)
        share_ref[...] = total * (1.0 / math.sqrt(rows * n_ba * n_aa))
    with jax.named_scope("w_last_sends"):
        landed(sibling_recv, everything).wait_send()

        def wait_relay(group, count):
            if count:
                relay_all(group, count).wait_send()

        for group in range(2):
            for_count(relays[group], functools.partial(wait_relay, group))
        remote_copy(tails, tails, small_send, tail_recv, {"ba": ba ^ 1}).wait_send()


def store(grad_vmem, share_vmem, grad_hbm, share_hbm, sem):
    rows = grad_vmem.shape[0] // STORES
    copies = [pltpu.make_async_copy(share_vmem, share_hbm, sem.at[1])]
    for index in range(STORES):
        block = pl.ds(index * rows, rows)
        copies.append(pltpu.make_async_copy(grad_vmem.at[block], grad_hbm.at[block], sem.at[0]))
    for copy in copies:
        copy.start()
    pltpu.make_async_copy(grad_vmem, grad_hbm, sem.at[0]).wait()
    copies[0].wait()


def fused(grad_out, saved_input, keep_bits, gain):
    n_ba, n_aa = lax.axis_size("ba"), lax.axis_size("aa")
    width = grad_out.shape[1]
    rows, depth = saved_input.shape
    n_direct, n_diagonal = len(steps_with(n_ba, 1)), len(steps_with(n_ba, 2))
    f32 = jnp.float32
    grad_in, share = pl.pallas_call(
        functools.partial(kernel, n_ba, n_aa),
        out_shape=(
            pltpu.VMEM((rows, depth), jnp.bfloat16),
            pltpu.VMEM((1, width), f32),
        ),
        in_specs=[pl.BlockSpec(memory_space=pl.ANY)] * 4,
        out_specs=(pl.BlockSpec(memory_space=pltpu.VMEM), pl.BlockSpec(memory_space=pltpu.VMEM)),
        scratch_shapes=[
            pltpu.VMEM((n_ba, rows, width), jnp.bfloat16),
            pltpu.VMEM((n_ba, rows, width), jnp.bfloat16),
            pltpu.VMEM((rows, depth), jnp.bfloat16),
            pltpu.VMEM(keep_bits.shape, jnp.int32),
            pltpu.VMEM((1, depth), f32),
            pltpu.VMEM((rows, depth), f32),
            pltpu.VMEM((rows, depth), f32),
            pltpu.VMEM((rows, LANES), f32),
            pltpu.VMEM((rows, LANES), f32),
            pltpu.VMEM((n_ba, 8, width), f32),
            pltpu.VMEM((n_ba, 1, width), f32),
            pltpu.VMEM((2, 1, width), f32),
            pltpu.VMEM((n_aa * (n_direct + n_diagonal + 1), 1, width), f32),
            pltpu.SemaphoreType.DMA,
            pltpu.SemaphoreType.DMA,
            pltpu.SemaphoreType.DMA,
            pltpu.SemaphoreType.DMA,
            pltpu.SemaphoreType.DMA((n_direct,)),
            pltpu.SemaphoreType.DMA((n_direct,)),
            pltpu.SemaphoreType.DMA,
            pltpu.SemaphoreType.DMA,
            pltpu.SemaphoreType.DMA,
            pltpu.SemaphoreType.DMA,
            pltpu.SemaphoreType.REGULAR,
            pltpu.SemaphoreType.REGULAR((n_aa - 1,)),
            pltpu.VMEM((2, 2, 2, 2, RELAY_ROWS, width), jnp.bfloat16),
            pltpu.SemaphoreType.DMA((2,)),
            pltpu.SemaphoreType.DMA((2,)),
            pltpu.SemaphoreType.DMA((2,)),
        ],
        compiler_params=pltpu.CompilerParams(collective_id=0, has_side_effects=True),
        name="regroup_backward",
    )(grad_out, saved_input, keep_bits, gain.reshape(1, depth))
    grad_in, share = pl.pallas_call(
        store,
        out_shape=(
            jax.ShapeDtypeStruct((rows, depth), jnp.bfloat16),
            jax.ShapeDtypeStruct((1, width), f32),
        ),
        in_specs=[pl.BlockSpec(memory_space=pltpu.VMEM)] * 2,
        out_specs=[pl.BlockSpec(memory_space=pl.ANY)] * 2,
        scratch_shapes=[pltpu.SemaphoreType.DMA((2,))],
        name="store_results",
    )(*(pltpu.with_memory_space_constraint(x, pltpu.VMEM) for x in (grad_in, share)))
    return (grad_in, share.reshape(width))


def per_device(grad_out, saved_input, keep_bits, gain):
    fits = grad_out.shape[1] % LANES == 0 and saved_input.shape[0] % CHUNK_ROWS == 0
    fits = fits and keep_bits.shape[1] == LANES
    n_ba = lax.axis_size("ba")
    fits = fits and n_ba & (n_ba - 1) == 0 and hops(n_ba - 1) == 2 and lax.axis_size("aa") > 1
    body = fused if fits else plain
    return body(grad_out, saved_input, keep_bits, gain)


def solution(mesh):
    placed = (P("aa", "ba"), P(("aa", "ba"), None), P(("aa", "ba"), None), P())
    return jax.shard_map(
        per_device,
        mesh=mesh,
        in_specs=placed,
        out_specs=(P(("aa", "ba"), None), P("ba")),
        check_vma=False,
    )
```

```python
import functools
import math

import jax
import jax.numpy as jnp
from jax import lax
from jax.experimental import pallas as pl
from jax.experimental.pallas import tpu as pltpu
from jax.sharding import PartitionSpec as P

KEEP_RATE = 0.9
EPSILON = 1e-06
LANES = 128
CHUNK_ROWS = 64
STORES = 4
FIRST_ROWS = 64
EARLY_ROWS = 48
RELAY_ROWS = 16
MESH = pl.DeviceIdType.MESH


def unpack_bits(words):
    shifts = jnp.arange(32, dtype=jnp.int32)
    bits = jnp.right_shift(words[:, :, None], shifts[None, None, :]) & 1
    return bits.reshape(words.shape[0], words.shape[1] * 32).astype(jnp.float32)


def rows_backward(grad_rows, input_rows, word_rows, gain):
    keep = unpack_bits(word_rows)
    dropped = input_rows.astype(jnp.float32) * keep * (1.0 / KEEP_RATE)
    inverse = lax.rsqrt(jnp.mean(dropped * dropped, axis=-1, keepdims=True) + EPSILON)
    normed = dropped * inverse
    grads = grad_rows.astype(jnp.float32)
    scaled = gain[None, :] * grads
    centre = jnp.mean(scaled * normed, axis=-1, keepdims=True)
    grad_in = (inverse * (scaled - normed * centre) * keep * (1.0 / KEEP_RATE)).astype(jnp.bfloat16)
    partial_sum = jnp.sum(grads * normed, axis=0)
    return (grad_in, partial_sum)


def plain(grad_out, saved_input, keep_bits, gain):
    groups = lax.axis_size("ba")
    rows = grad_out.shape[0] // groups
    pieces = grad_out.reshape(groups, rows, grad_out.shape[1])
    arrived = lax.all_to_all(pieces, "ba", split_axis=0, concat_axis=2, tiled=True)
    grad_rows = arrived.reshape(rows, arrived.shape[2])
    grad_in, partial_sum = rows_backward(grad_rows, saved_input, keep_bits, gain)
    total_tokens = rows * groups * lax.axis_size("aa")
    owned = lax.psum_scatter(partial_sum, "ba", scatter_dimension=0, tiled=True)
    share = lax.psum(owned, "aa")
    gain_grad = share * (1.0 / math.sqrt(total_tokens))
    return (grad_in, gain_grad)


def hops(step):
    return (step >> 1).bit_count()


def steps_with(n_ba, count):
    return sorted((step for step in range(n_ba) if hops(step) == count), key=lambda step: (step % 2, step))


def kernel(n_ba, n_aa, grad_hbm, input_hbm, bits_hbm, gain_hbm, out_ref, share_ref,
           staged, arrived, held, words, gain_ref, normed, masked_gain, outer, totals, sums,
           parts, slices, tails, stage_sem, load_sem, send_sem, small_send, early_recv,
           last_recv, diagonal_recv, sibling_recv, part_recv, tail_recv, ready, flood,
           relayed, relay_recv, relay_send, corner_recv):
    ba, aa = lax.axis_index("ba"), lax.axis_index("aa")
    rows, width = arrived.shape[1], arrived.shape[2]
    depth = n_ba * width
    chunks = rows // CHUNK_ROWS
    tiles = width // LANES
    direct, diagonal = steps_with(n_ba, 1), steps_with(n_ba, 2)
    n_direct, n_diagonal = len(direct), len(diagonal)
    half = n_direct // 2
    per_plane = n_direct + n_diagonal + 1
    order = [0, 1] + direct + diagonal
    slot = {step: place for place, step in enumerate(order)}
    swap = lax.rem(ba // (2 * direct[0]), 2)
    arrivals = [
        (side + offset, 2 + (half if side else 0) + index)
        for offset, index in ((2 + 2 * swap, swap), (4 - 2 * swap, 1 - swap))
        for side in range(2)
    ]
    groups = (arrivals[:half], arrivals[half:])
    early = (0, EARLY_ROWS)
    first_chip = ba < 2
    beside = (ba ^ groups[0][0][0]) < 2
    never = ba < 0

    def amounts(plane, near_first):
        top = plane == n_aa - 1
        second = plane == n_aa - 2 if n_aa > 3 else never
        both = jnp.logical_and
        one = jnp.logical_or(both(top, jnp.logical_not(near_first)), both(second, near_first))
        return {1: one, 2: both(top, near_first)}

    mirror = n_aa - 1 - aa
    odd = lax.rem(ba, 2) == 1
    sends = amounts(aa, first_chip)
    fed = (amounts(aa, beside), amounts(aa, never))
    relays = tuple(
        {count: jnp.logical_and(flag, odd) for count, flag in amounts(mirror, near).items()}
        for near in (beside, never)
    )

    def either(flags):
        return jnp.logical_or(flags[1], flags[2])

    def last(count):
        return (EARLY_ROWS, rows - EARLY_ROWS - count * RELAY_ROWS)

    def relay_block(index, count=1):
        return pl.ds(rows - (index + count) * RELAY_ROWS, count * RELAY_ROWS)

    def for_count(flags, action):
        for count, flag in flags.items():
            pl.when(flag)(functools.partial(action, count))
        pl.when(jnp.logical_not(either(flags)))(functools.partial(action, 0))

    def remote_copy(source, target, send, recv, device):
        return pltpu.make_async_remote_copy(
            src_ref=source, dst_ref=target, send_sem=send, recv_sem=recv,
            device_id=device, device_id_type=MESH,
        )

    def column(step):
        return lax.rem(aa + step, n_aa)

    def rows_of(chunk):
        start = chunk * CHUNK_ROWS
        if not isinstance(start, int):
            start = pl.multiple_of(start, CHUNK_ROWS)
        return pl.ds(start, CHUNK_ROWS)

    def stage(step, semaphore):
        first = pl.ds(pl.multiple_of((ba ^ step) * rows, CHUNK_ROWS), rows)
        target = staged.at[slot[step]] if step else arrived.at[0]
        return pltpu.make_async_copy(grad_hbm.at[first], target, semaphore)

    def piece(step, recv, block=None, place=None):
        place = slot[step] if place is None else place
        at = (place, pl.ds(*block)) if block else (place,)
        return remote_copy(staged.at[at], arrived.at[at], send_sem, recv, {"ba": ba ^ step})

    def axis_of(step):
        return 1 if step >= 2 * direct[0] else 0

    def early_piece(step):
        return piece(step, early_recv.at[axis_of(step)], early)

    def last_piece(step, block):
        return piece(step, last_recv.at[axis_of(step)], block)

    def to_relay(step, index):
        target = ba ^ step
        parity = lax.rem(target, 2)
        swapped = lax.rem(target // (2 * direct[0]), 2)
        group = 1 - swapped if axis_of(step) else swapped
        return remote_copy(
            staged.at[slot[step], relay_block(index)], relayed.at[group, index, parity, step % 2],
            send_sem, relay_recv.at[group], {"aa": mirror, "ba": target + 1 - parity},
        )

    def from_relay(group, index, parity, cross):
        return remote_copy(
            relayed.at[group, index, parity, cross], arrived.at[groups[group][cross][1], relay_block(index)],
            relay_send.at[group], corner_recv.at[group], {"aa": mirror, "ba": ba - 1 + parity},
        )

    def relay_all(group, count):
        blocks = relayed.at[group, pl.ds(0, count)]
        return remote_copy(blocks, blocks, relay_send.at[group], relay_recv.at[group], {"ba": ba ^ 1})

    def landed(recv, *at):
        return remote_copy(staged.at[at], arrived.at[at], send_sem, recv, {"ba": ba ^ 1})

    def part():
        return remote_copy(parts.at[1], slices.at[1], small_send, part_recv, {"ba": ba ^ 1})

    def share(step):
        mine = tails.at[aa * per_plane]
        return remote_copy(mine, mine, small_send, tail_recv, {"aa": column(step)})

    def late(target, step, place):
        return remote_copy(
            parts.at[place], tails.at[aa * per_plane + place - 1], small_send, tail_recv,
            {"aa": target, "ba": ba ^ step},
        )

    def greet_column(semaphore):
        @pl.when(aa > 0)
        def _():
            pl.semaphore_signal(semaphore, inc=1, device_id={"aa": aa - 1}, device_id_type=MESH)

        @pl.when(aa < n_aa - 1)
        def _():
            pl.semaphore_signal(semaphore, inc=1, device_id={"aa": aa + 1}, device_id_type=MESH)

    column_peers = (aa > 0).astype(jnp.int32) + (aa < n_aa - 1).astype(jnp.int32)

    barrier = pltpu.get_barrier_semaphore()
    for step in direct + [1]:
        pl.semaphore_signal(barrier, inc=1, device_id={"ba": ba ^ step}, device_id_type=MESH)
    greet_column(barrier)

    for group in range(2):
        @pl.when(either(relays[group]))
        def _(group=group):
            for step, _ in groups[group]:
                pl.semaphore_signal(
                    barrier, inc=1, device_id={"aa": mirror, "ba": ba ^ step}, device_id_type=MESH)

    for step in order[1:]:
        stage(step, stage_sem).start()
    loads = [
        pltpu.make_async_copy(bits_hbm, words, load_sem),
        pltpu.make_async_copy(gain_hbm, gain_ref, load_sem),
        pltpu.make_async_copy(input_hbm, held, load_sem),
        stage(0, load_sem),
    ]
    for load in loads:
        load.start()
    with jax.named_scope("w_barrier"):
        pl.semaphore_wait(barrier, n_direct + 1 + column_peers + half * either(sends).astype(jnp.int32))
    pl.semaphore_signal(ready, inc=1, device_id={"ba": ba ^ direct[0]}, device_id_type=MESH)
    with jax.named_scope("w_stage"):
        everything = pl.ds(1, n_ba - 1)
        pltpu.make_async_copy(staged.at[everything], staged.at[everything], stage_sem).wait()
    for step in direct:
        early_piece(step).start()

    @pl.when(either(sends))
    def _():
        for step in direct:
            to_relay(step, 0).start()

    @pl.when(sends[2])
    def _():
        for step in direct:
            to_relay(step, 1).start()

    piece(1, sibling_recv).start()
    with jax.named_scope("w_ready"):
        pl.semaphore_wait(ready, 1)
    greet_column(flood.at[0])
    for step in diagonal:
        piece(step, diagonal_recv).start()

    def start_last(count):
        for step in direct:
            last_piece(step, last(count)).start()

    for_count(sends, start_last)
    with jax.named_scope("w_load"):
        for load in loads:
            load.wait()

    lane = lax.broadcasted_iota(jnp.int32, (CHUNK_ROWS, LANES), 1)
    word_of = lane // 32
    flag = jnp.left_shift(jnp.int32(1), lane % 32)

    def span(source, tile):
        return pl.ds(pl.multiple_of(source * width + tile * LANES, LANES), LANES)

    def prepare(chunk, carry):
        block = rows_of(chunk)

        def drop(source, squares):
            row_words = words[block, :]
            for tile in range(tiles):
                at = span(source, tile)
                index = word_of + (source * tiles + tile) * (LANES // 32)
                spread = jnp.take_along_axis(row_words, index, axis=1, mode="promise_in_bounds")
                kept = (spread & flag) != 0
                dropped = jnp.where(kept, held[block, at].astype(jnp.float32), 0.0) * (1.0 / KEEP_RATE)
                normed[block, at] = dropped
                masked_gain[block, at] = jnp.where(kept, gain_ref[:, at], 0.0)
                squares = squares + dropped * dropped
            return squares

        squares = lax.fori_loop(0, n_ba, drop, jnp.zeros((CHUNK_ROWS, LANES), jnp.float32))
        mean = jnp.sum(squares, axis=1, keepdims=True) * (1.0 / depth)
        inverse = lax.rsqrt(mean + EPSILON)
        outer[block, :] = jnp.broadcast_to(inverse * (1.0 / KEEP_RATE), (CHUNK_ROWS, LANES))

        def scale(source, none):
            for tile in range(tiles):
                at = span(source, tile)
                normed[block, at] = normed[block, at] * inverse
            return none

        lax.fori_loop(0, n_ba, scale, 0)
        return carry

    with jax.named_scope("prepare"):
        lax.fori_loop(0, chunks, prepare, 0)
    sums[...] = jnp.zeros_like(sums)
    totals[...] = jnp.zeros_like(totals)

    def first(step, place, start, size):
        source, count = ba ^ step, math.gcd(start, size, FIRST_ROWS)

        def some(index, none):
            block = pl.ds(pl.multiple_of(start + index * count, count), count)
            total = totals[block, :]
            for tile in range(tiles):
                at = span(source, tile)
                here = slice(tile * LANES, (tile + 1) * LANES)
                grads = arrived[place, block, here].astype(jnp.float32)
                product = grads * normed[block, at]
                total = total + product * gain_ref[:, at]
                sums[place, :, here] += jnp.sum(product.reshape(count // 8, 8, LANES), axis=0)
            totals[block, :] = total
            return none

        lax.fori_loop(0, size // count, some, 0)

    def finish(chunk, none):
        block = rows_of(chunk)
        factor = outer[block, :]
        centre = jnp.sum(totals[block, :], axis=1, keepdims=True) * (1.0 / depth)

        for step in order:
            for tile in range(tiles):
                at = span(ba ^ step, tile)
                grads = arrived[slot[step], block, tile * LANES:(tile + 1) * LANES].astype(jnp.float32)
                value = factor * (masked_gain[block, at] * grads - normed[block, at] * centre)
                out_ref[block, at] = value.astype(jnp.bfloat16)
        return none

    def fold(place):
        return jnp.sum(sums[place], axis=0, keepdims=True)

    def send_late(step, place):
        parts[place] = fold(place)
        for target in range(n_aa):
            late(target, step, place).start()

    def meet(turn):
        with jax.named_scope(f"w_flood{turn}"):
            pl.semaphore_wait(flood.at[turn], column_peers)
        if turn < n_aa - 2:
            greet_column(flood.at[turn + 1])

    axes = (swap, 1 - swap)

    def take_early(group):
        with jax.named_scope("w_early"):
            landed(early_recv.at[axes[group]], pl.ds(2, half), pl.ds(*early)).wait_recv()
        for step, place in groups[group]:
            first(step, place, *early)

    first(0, 0, 0, rows)
    slices[0] = fold(0)
    with jax.named_scope("w_sibling"):
        piece(1, sibling_recv).wait_recv()
    first(1, 1, 0, rows)
    parts[1] = fold(1)
    part().start()
    meet(0)

    def pass_on(group, count):
        if count:
            with jax.named_scope("w_relay"):
                relay_all(group, count).wait_recv()
            for index in range(count):
                for parity in range(2):
                    for cross in range(2):
                        from_relay(group, index, parity, cross).start()

    for group in range(2):
        for_count(relays[group], functools.partial(pass_on, group))
    for turn in range(1, n_aa - 1):
        meet(turn)
    with jax.named_scope("w_part"):
        part().wait_recv()
    tails[aa * per_plane] = slices[0] + slices[1]
    for step in range(1, n_aa):
        share(step).start()
    def take_diagonal():
        with jax.named_scope("w_diag"):
            landed(diagonal_recv, pl.ds(2 + n_direct, n_diagonal)).wait_recv()
        for step in diagonal:
            first(step, slot[step], 0, rows)
            send_late(step, slot[step])

    def take_group(group, count):
        if count:
            with jax.named_scope("w_corner"):
                landed(corner_recv.at[group], pl.ds(2, half), relay_block(0, count)).wait_recv()
            for step, place in groups[group]:
                first(step, place, rows - count * RELAY_ROWS, count * RELAY_ROWS)
        with jax.named_scope("w_last"):
            landed(last_recv.at[axes[group]], pl.ds(2, half), pl.ds(*last(count))).wait_recv()
        for cross in (0, 1):
            step, place = groups[group][cross]
            first(step, place, *last(count))
            send_late(step, place)

    pl.when(jnp.logical_not(beside))(take_diagonal)
    take_early(0)
    for_count(fed[0], functools.partial(take_group, 0))
    pl.when(beside)(take_diagonal)
    take_early(1)
    for_count(fed[1], functools.partial(take_group, 1))
    with jax.named_scope("finish"):
        lax.fori_loop(0, chunks, finish, 0)
    with jax.named_scope("w_tail"):
        others = tails.at[pl.ds(0, n_aa * per_plane - 1)]
        remote_copy(others, others, small_send, tail_recv, {"ba": ba ^ 1}).wait_recv()
    with jax.named_scope("final_sum"):
        total = jnp.sum(tails[...], axis=0)
        share_ref[...] = total * (1.0 / math.sqrt(rows * n_ba * n_aa))
    with jax.named_scope("w_last_sends"):
        landed(sibling_recv, everything).wait_send()

        def wait_relay(group, count):
            if count:
                relay_all(group, count).wait_send()

        for group in range(2):
            for_count(relays[group], functools.partial(wait_relay, group))
        remote_copy(tails, tails, small_send, tail_recv, {"ba": ba ^ 1}).wait_send()


def store(grad_vmem, share_vmem, grad_hbm, share_hbm, sem):
    rows = grad_vmem.shape[0] // STORES
    copies = [pltpu.make_async_copy(share_vmem, share_hbm, sem.at[1])]
    for index in range(STORES):
        block = pl.ds(index * rows, rows)
        copies.append(pltpu.make_async_copy(grad_vmem.at[block], grad_hbm.at[block], sem.at[0]))
    for copy in copies:
        copy.start()
    pltpu.make_async_copy(grad_vmem, grad_hbm, sem.at[0]).wait()
    copies[0].wait()


def fused(grad_out, saved_input, keep_bits, gain):
    n_ba, n_aa = lax.axis_size("ba"), lax.axis_size("aa")
    width = grad_out.shape[1]
    rows, depth = saved_input.shape
    n_direct, n_diagonal = len(steps_with(n_ba, 1)), len(steps_with(n_ba, 2))
    f32 = jnp.float32
    grad_in, share = pl.pallas_call(
        functools.partial(kernel, n_ba, n_aa),
        out_shape=(
            pltpu.VMEM((rows, depth), jnp.bfloat16),
            pltpu.VMEM((1, width), f32),
        ),
        in_specs=[pl.BlockSpec(memory_space=pl.ANY)] * 4,
        out_specs=(pl.BlockSpec(memory_space=pltpu.VMEM), pl.BlockSpec(memory_space=pltpu.VMEM)),
        scratch_shapes=[
            pltpu.VMEM((n_ba, rows, width), jnp.bfloat16),
            pltpu.VMEM((n_ba, rows, width), jnp.bfloat16),
            pltpu.VMEM((rows, depth), jnp.bfloat16),
            pltpu.VMEM(keep_bits.shape, jnp.int32),
            pltpu.VMEM((1, depth), f32),
            pltpu.VMEM((rows, depth), f32),
            pltpu.VMEM((rows, depth), f32),
            pltpu.VMEM((rows, LANES), f32),
            pltpu.VMEM((rows, LANES), f32),
            pltpu.VMEM((n_ba, 8, width), f32),
            pltpu.VMEM((n_ba, 1, width), f32),
            pltpu.VMEM((2, 1, width), f32),
            pltpu.VMEM((n_aa * (n_direct + n_diagonal + 1), 1, width), f32),
            pltpu.SemaphoreType.DMA,
            pltpu.SemaphoreType.DMA,
            pltpu.SemaphoreType.DMA,
            pltpu.SemaphoreType.DMA,
            pltpu.SemaphoreType.DMA((2,)),
            pltpu.SemaphoreType.DMA((2,)),
            pltpu.SemaphoreType.DMA,
            pltpu.SemaphoreType.DMA,
            pltpu.SemaphoreType.DMA,
            pltpu.SemaphoreType.DMA,
            pltpu.SemaphoreType.REGULAR,
            pltpu.SemaphoreType.REGULAR((n_aa - 1,)),
            pltpu.VMEM((2, 2, 2, 2, RELAY_ROWS, width), jnp.bfloat16),
            pltpu.SemaphoreType.DMA((2,)),
            pltpu.SemaphoreType.DMA((2,)),
            pltpu.SemaphoreType.DMA((2,)),
        ],
        compiler_params=pltpu.CompilerParams(collective_id=0, has_side_effects=True),
        name="regroup_backward",
    )(grad_out, saved_input, keep_bits, gain.reshape(1, depth))
    grad_in, share = pl.pallas_call(
        store,
        out_shape=(
            jax.ShapeDtypeStruct((rows, depth), jnp.bfloat16),
            jax.ShapeDtypeStruct((1, width), f32),
        ),
        in_specs=[pl.BlockSpec(memory_space=pltpu.VMEM)] * 2,
        out_specs=[pl.BlockSpec(memory_space=pl.ANY)] * 2,
        scratch_shapes=[pltpu.SemaphoreType.DMA((2,))],
        name="store_results",
    )(*(pltpu.with_memory_space_constraint(x, pltpu.VMEM) for x in (grad_in, share)))
    return (grad_in, share.reshape(width))


def per_device(grad_out, saved_input, keep_bits, gain):
    fits = grad_out.shape[1] % LANES == 0 and saved_input.shape[0] % CHUNK_ROWS == 0
    fits = fits and keep_bits.shape[1] == LANES
    n_ba = lax.axis_size("ba")
    fits = fits and n_ba & (n_ba - 1) == 0 and hops(n_ba - 1) == 2 and lax.axis_size("aa") > 1
    body = fused if fits else plain
    return body(grad_out, saved_input, keep_bits, gain)


def solution(mesh):
    placed = (P("aa", "ba"), P(("aa", "ba"), None), P(("aa", "ba"), None), P())
    return jax.shard_map(
        per_device,
        mesh=mesh,
        in_specs=placed,
        out_specs=(P(("aa", "ba"), None), P("ba")),
        check_vma=False,
    )
```

```python
import functools
import math

import jax
import jax.numpy as jnp
from jax import lax
from jax.experimental import pallas as pl
from jax.experimental.pallas import tpu as pltpu
from jax.sharding import PartitionSpec as P

KEEP_RATE = 0.9
EPSILON = 1e-06
LANES = 128
CHUNK_ROWS = 64
STORES = 4
FIRST_ROWS = 64
EARLY_ROWS = 48
RELAY_ROWS = 16
RELAYED = ((2, 2), (1, 1), (1, 1))
MESH = pl.DeviceIdType.MESH


def unpack_bits(words):
    shifts = jnp.arange(32, dtype=jnp.int32)
    bits = jnp.right_shift(words[:, :, None], shifts[None, None, :]) & 1
    return bits.reshape(words.shape[0], words.shape[1] * 32).astype(jnp.float32)


def rows_backward(grad_rows, input_rows, word_rows, gain):
    keep = unpack_bits(word_rows)
    dropped = input_rows.astype(jnp.float32) * keep * (1.0 / KEEP_RATE)
    inverse = lax.rsqrt(jnp.mean(dropped * dropped, axis=-1, keepdims=True) + EPSILON)
    normed = dropped * inverse
    grads = grad_rows.astype(jnp.float32)
    scaled = gain[None, :] * grads
    centre = jnp.mean(scaled * normed, axis=-1, keepdims=True)
    grad_in = (inverse * (scaled - normed * centre) * keep * (1.0 / KEEP_RATE)).astype(jnp.bfloat16)
    partial_sum = jnp.sum(grads * normed, axis=0)
    return (grad_in, partial_sum)


def plain(grad_out, saved_input, keep_bits, gain):
    groups = lax.axis_size("ba")
    rows = grad_out.shape[0] // groups
    pieces = grad_out.reshape(groups, rows, grad_out.shape[1])
    arrived = lax.all_to_all(pieces, "ba", split_axis=0, concat_axis=2, tiled=True)
    grad_rows = arrived.reshape(rows, arrived.shape[2])
    grad_in, partial_sum = rows_backward(grad_rows, saved_input, keep_bits, gain)
    total_tokens = rows * groups * lax.axis_size("aa")
    owned = lax.psum_scatter(partial_sum, "ba", scatter_dimension=0, tiled=True)
    share = lax.psum(owned, "aa")
    gain_grad = share * (1.0 / math.sqrt(total_tokens))
    return (grad_in, gain_grad)


def hops(step):
    return (step >> 1).bit_count()


def steps_with(n_ba, count):
    return sorted((step for step in range(n_ba) if hops(step) == count), key=lambda step: (step % 2, step))


def kernel(n_ba, n_aa, grad_hbm, input_hbm, bits_hbm, gain_hbm, out_ref, share_ref,
           staged, arrived, held, words, gain_ref, normed, masked_gain, outer, totals, sums,
           parts, slices, tails, stage_sem, load_sem, send_sem, small_send, early_recv,
           last_recv, diagonal_recv, sibling_recv, part_recv, tail_recv, ready, flood,
           relayed, relay_recv, relay_send, corner_recv):
    ba, aa = lax.axis_index("ba"), lax.axis_index("aa")
    rows, width = arrived.shape[1], arrived.shape[2]
    depth = n_ba * width
    chunks = rows // CHUNK_ROWS
    tiles = width // LANES
    direct, diagonal = steps_with(n_ba, 1), steps_with(n_ba, 2)
    n_direct, n_diagonal = len(direct), len(diagonal)
    half = n_direct // 2
    per_plane = n_direct + n_diagonal + 1
    order = [0, 1] + direct + diagonal
    slot = {step: place for place, step in enumerate(order)}
    swap = lax.rem(ba // (2 * direct[0]), 2)
    arrivals = [
        (side + offset, 2 + (half if side else 0) + index)
        for offset, index in ((2 + 2 * swap, swap), (4 - 2 * swap, 1 - swap))
        for side in range(2)
    ]
    groups = (arrivals[:half], arrivals[half:])
    early = (0, EARLY_ROWS)
    first_chip = ba < 2
    beside = (ba ^ groups[0][0][0]) < 2
    never = ba < 0

    def kinds(plane, near_first):
        top = plane == n_aa - 1
        second = plane == n_aa - 2 if n_aa > 3 else never
        both = jnp.logical_and
        return (both(top, near_first), both(second, near_first), both(top, jnp.logical_not(near_first)))

    mirror = n_aa - 1 - aa
    odd = lax.rem(ba, 2) == 1
    sends = kinds(aa, first_chip)
    fed = (kinds(aa, beside), kinds(aa, never))
    relays = tuple(
        tuple(jnp.logical_and(flag, odd) for flag in kinds(mirror, near)) for near in (beside, never)
    )

    def either(flags):
        return jnp.logical_or(jnp.logical_or(flags[0], flags[1]), flags[2])

    def last(count):
        return (EARLY_ROWS, rows - EARLY_ROWS - count * RELAY_ROWS)

    def relay_block(index, count=1):
        return pl.ds(rows - (index + count) * RELAY_ROWS, count * RELAY_ROWS)

    def for_kind(flags, action):
        for blocks, flag in zip(RELAYED, flags):
            pl.when(flag)(functools.partial(action, blocks))
        pl.when(jnp.logical_not(either(flags)))(functools.partial(action, (0, 0)))

    def for_core(blocks, action):
        if blocks[0] == blocks[1]:
            action(blocks[0])
        else:
            pl.when(odd)(functools.partial(action, blocks[1]))
            pl.when(jnp.logical_not(odd))(functools.partial(action, blocks[0]))

    def remote_copy(source, target, send, recv, device):
        return pltpu.make_async_remote_copy(
            src_ref=source, dst_ref=target, send_sem=send, recv_sem=recv,
            device_id=device, device_id_type=MESH,
        )

    def column(step):
        return lax.rem(aa + step, n_aa)

    def rows_of(chunk):
        start = chunk * CHUNK_ROWS
        if not isinstance(start, int):
            start = pl.multiple_of(start, CHUNK_ROWS)
        return pl.ds(start, CHUNK_ROWS)

    def stage(step, semaphore):
        first = pl.ds(pl.multiple_of((ba ^ step) * rows, CHUNK_ROWS), rows)
        target = staged.at[slot[step]] if step else arrived.at[0]
        return pltpu.make_async_copy(grad_hbm.at[first], target, semaphore)

    def piece(step, recv, block=None, place=None):
        place = slot[step] if place is None else place
        at = (place, pl.ds(*block)) if block else (place,)
        return remote_copy(staged.at[at], arrived.at[at], send_sem, recv, {"ba": ba ^ step})

    def axis_of(step):
        return 1 if step >= 2 * direct[0] else 0

    def early_piece(step):
        return piece(step, early_recv.at[axis_of(step)], early)

    def last_piece(step, block):
        return piece(step, last_recv.at[axis_of(step)], block)

    def to_relay(step, index):
        target = ba ^ step
        parity = lax.rem(target, 2)
        swapped = lax.rem(target // (2 * direct[0]), 2)
        group = 1 - swapped if axis_of(step) else swapped
        return remote_copy(
            staged.at[slot[step], relay_block(index)], relayed.at[group, index, parity, step % 2],
            send_sem, relay_recv.at[group], {"aa": mirror, "ba": target + 1 - parity},
        )

    def from_relay(group, index, parity, cross):
        return remote_copy(
            relayed.at[group, index, parity, cross], arrived.at[groups[group][cross][1], relay_block(index)],
            relay_send.at[group], corner_recv.at[group], {"aa": mirror, "ba": ba - 1 + parity},
        )

    def relay_all(group, count):
        blocks = relayed.at[group, pl.ds(0, count)]
        return remote_copy(blocks, blocks, relay_send.at[group], relay_recv.at[group], {"ba": ba ^ 1})

    def landed(recv, *at):
        return remote_copy(staged.at[at], arrived.at[at], send_sem, recv, {"ba": ba ^ 1})

    def part():
        return remote_copy(parts.at[1], slices.at[1], small_send, part_recv, {"ba": ba ^ 1})

    def share(step):
        mine = tails.at[aa * per_plane]
        return remote_copy(mine, mine, small_send, tail_recv, {"aa": column(step)})

    def late(target, step, place):
        return remote_copy(
            parts.at[place], tails.at[aa * per_plane + place - 1], small_send, tail_recv,
            {"aa": target, "ba": ba ^ step},
        )

    def greet_column(semaphore):
        @pl.when(aa > 0)
        def _():
            pl.semaphore_signal(semaphore, inc=1, device_id={"aa": aa - 1}, device_id_type=MESH)

        @pl.when(aa < n_aa - 1)
        def _():
            pl.semaphore_signal(semaphore, inc=1, device_id={"aa": aa + 1}, device_id_type=MESH)

    column_peers = (aa > 0).astype(jnp.int32) + (aa < n_aa - 1).astype(jnp.int32)

    barrier = pltpu.get_barrier_semaphore()
    for step in direct + [1]:
        pl.semaphore_signal(barrier, inc=1, device_id={"ba": ba ^ step}, device_id_type=MESH)
    greet_column(barrier)

    for group in range(2):
        @pl.when(either(relays[group]))
        def _(group=group):
            for step, _ in groups[group]:
                pl.semaphore_signal(
                    barrier, inc=1, device_id={"aa": mirror, "ba": ba ^ step}, device_id_type=MESH)

    for step in order[1:]:
        stage(step, stage_sem).start()
    loads = [
        pltpu.make_async_copy(bits_hbm, words, load_sem),
        pltpu.make_async_copy(gain_hbm, gain_ref, load_sem),
        pltpu.make_async_copy(input_hbm, held, load_sem),
        stage(0, load_sem),
    ]
    for load in loads:
        load.start()
    with jax.named_scope("w_barrier"):
        pl.semaphore_wait(barrier, n_direct + 1 + column_peers + half * either(sends).astype(jnp.int32))
    pl.semaphore_signal(ready, inc=1, device_id={"ba": ba ^ direct[0]}, device_id_type=MESH)
    with jax.named_scope("w_stage"):
        everything = pl.ds(1, n_ba - 1)
        pltpu.make_async_copy(staged.at[everything], staged.at[everything], stage_sem).wait()
    for step in direct:
        early_piece(step).start()

    def start_relays(blocks):
        def start(count):
            for index in range(count):
                for step in direct:
                    to_relay(step, index).start()

        for_core(blocks, start)

    for_kind(sends, start_relays)

    piece(1, sibling_recv).start()
    with jax.named_scope("w_ready"):
        pl.semaphore_wait(ready, 1)
    greet_column(flood.at[0])
    for step in diagonal:
        piece(step, diagonal_recv).start()

    def start_last(blocks):
        def start(count):
            for step in direct:
                last_piece(step, last(count)).start()

        for_core(blocks, start)

    for_kind(sends, start_last)
    with jax.named_scope("w_load"):
        for load in loads:
            load.wait()

    lane = lax.broadcasted_iota(jnp.int32, (CHUNK_ROWS, LANES), 1)
    word_of = lane // 32
    flag = jnp.left_shift(jnp.int32(1), lane % 32)

    def span(source, tile):
        return pl.ds(pl.multiple_of(source * width + tile * LANES, LANES), LANES)

    def prepare(chunk, carry):
        block = rows_of(chunk)

        def drop(source, squares):
            row_words = words[block, :]
            for tile in range(tiles):
                at = span(source, tile)
                index = word_of + (source * tiles + tile) * (LANES // 32)
                spread = jnp.take_along_axis(row_words, index, axis=1, mode="promise_in_bounds")
                kept = (spread & flag) != 0
                dropped = jnp.where(kept, held[block, at].astype(jnp.float32), 0.0) * (1.0 / KEEP_RATE)
                normed[block, at] = dropped
                masked_gain[block, at] = jnp.where(kept, gain_ref[:, at], 0.0)
                squares = squares + dropped * dropped
            return squares

        squares = lax.fori_loop(0, n_ba, drop, jnp.zeros((CHUNK_ROWS, LANES), jnp.float32))
        mean = jnp.sum(squares, axis=1, keepdims=True) * (1.0 / depth)
        inverse = lax.rsqrt(mean + EPSILON)
        outer[block, :] = jnp.broadcast_to(inverse * (1.0 / KEEP_RATE), (CHUNK_ROWS, LANES))

        def scale(source, none):
            for tile in range(tiles):
                at = span(source, tile)
                normed[block, at] = normed[block, at] * inverse
            return none

        lax.fori_loop(0, n_ba, scale, 0)
        return carry

    with jax.named_scope("prepare"):
        lax.fori_loop(0, chunks, prepare, 0)
    sums[...] = jnp.zeros_like(sums)
    totals[...] = jnp.zeros_like(totals)

    def first(step, place, start, size):
        source = ba ^ step

        def some(block, count):
            total = totals[block, :]
            for tile in range(tiles):
                at = span(source, tile)
                here = slice(tile * LANES, (tile + 1) * LANES)
                grads = arrived[place, block, here].astype(jnp.float32)
                product = grads * normed[block, at]
                total = total + product * gain_ref[:, at]
                sums[place, :, here] += jnp.sum(product.reshape(count // 8, 8, LANES), axis=0)
            totals[block, :] = total

        if size % FIRST_ROWS:
            some(pl.ds(start, size), size)
        else:
            def more(index, none):
                some(pl.ds(pl.multiple_of(start + index * FIRST_ROWS, RELAY_ROWS), FIRST_ROWS), FIRST_ROWS)
                return none

            lax.fori_loop(0, size // FIRST_ROWS, more, 0)

    def finish(chunk, none):
        block = rows_of(chunk)
        factor = outer[block, :]
        centre = jnp.sum(totals[block, :], axis=1, keepdims=True) * (1.0 / depth)

        for step in order:
            for tile in range(tiles):
                at = span(ba ^ step, tile)
                grads = arrived[slot[step], block, tile * LANES:(tile + 1) * LANES].astype(jnp.float32)
                value = factor * (masked_gain[block, at] * grads - normed[block, at] * centre)
                out_ref[block, at] = value.astype(jnp.bfloat16)
        return none

    def fold(place):
        return jnp.sum(sums[place], axis=0, keepdims=True)

    def send_late(step, place):
        parts[place] = fold(place)
        for target in range(n_aa):
            late(target, step, place).start()

    def meet(turn):
        with jax.named_scope(f"w_flood{turn}"):
            pl.semaphore_wait(flood.at[turn], column_peers)
        if turn < n_aa - 2:
            greet_column(flood.at[turn + 1])

    axes = (swap, 1 - swap)

    def take_early(group):
        with jax.named_scope("w_early"):
            landed(early_recv.at[axes[group]], pl.ds(2, half), pl.ds(*early)).wait_recv()
        for step, place in groups[group]:
            first(step, place, *early)

    first(0, 0, 0, rows)
    slices[0] = fold(0)
    with jax.named_scope("w_sibling"):
        piece(1, sibling_recv).wait_recv()
    first(1, 1, 0, rows)
    parts[1] = fold(1)
    part().start()
    meet(0)

    def pass_on(group, blocks):
        if sum(blocks):
            with jax.named_scope("w_relay"):
                relay_all(group, sum(blocks) // 2).wait_recv()
            for parity in range(2):
                for cross in range(2):
                    for index in range(blocks[parity ^ cross]):
                        from_relay(group, index, parity, cross).start()

    for team in range(2):
        for_kind(relays[team], functools.partial(pass_on, team))
    for turn in range(1, n_aa - 1):
        meet(turn)
    with jax.named_scope("w_part"):
        part().wait_recv()
    tails[aa * per_plane] = slices[0] + slices[1]
    for step in range(1, n_aa):
        share(step).start()
    def take_diagonal():
        with jax.named_scope("w_diag"):
            landed(diagonal_recv, pl.ds(2 + n_direct, n_diagonal)).wait_recv()
        for step in diagonal:
            first(step, slot[step], 0, rows)
            send_late(step, slot[step])

    def land_group(group, blocks):
        count = sum(blocks) // 2
        if count:
            with jax.named_scope("w_corner"):
                landed(corner_recv.at[group], pl.ds(2, half), relay_block(0, count)).wait_recv()
        with jax.named_scope("w_last"):
            landed(last_recv.at[axes[group]], pl.ds(2, half), pl.ds(*last(count))).wait_recv()

    def take_group(group):
        for_kind(fed[group], functools.partial(land_group, group))
        for turn in range(2):
            cross = lax.rem(ba + turn, 2)
            step, place = groups[group][0][0] + cross, groups[group][0][1] + half * cross
            first(step, place, EARLY_ROWS, rows - EARLY_ROWS)
            send_late(step, place)

    pl.when(jnp.logical_not(beside))(take_diagonal)
    take_early(0)
    take_group(0)
    pl.when(beside)(take_diagonal)
    take_early(1)
    take_group(1)
    with jax.named_scope("finish"):
        lax.fori_loop(0, chunks, finish, 0)
    with jax.named_scope("w_tail"):
        others = tails.at[pl.ds(0, n_aa * per_plane - 1)]
        remote_copy(others, others, small_send, tail_recv, {"ba": ba ^ 1}).wait_recv()
    with jax.named_scope("final_sum"):
        total = jnp.sum(tails[...], axis=0)
        share_ref[...] = total * (1.0 / math.sqrt(rows * n_ba * n_aa))
    with jax.named_scope("w_last_sends"):
        landed(sibling_recv, everything).wait_send()

        def wait_relay(group, blocks):
            if sum(blocks):
                relay_all(group, sum(blocks) // 2).wait_send()

        for team in range(2):
            for_kind(relays[team], functools.partial(wait_relay, team))

        remote_copy(tails, tails, small_send, tail_recv, {"ba": ba ^ 1}).wait_send()


def store(grad_vmem, share_vmem, grad_hbm, share_hbm, sem):
    rows = grad_vmem.shape[0] // STORES
    copies = [pltpu.make_async_copy(share_vmem, share_hbm, sem.at[1])]
    for index in range(STORES):
        block = pl.ds(index * rows, rows)
        copies.append(pltpu.make_async_copy(grad_vmem.at[block], grad_hbm.at[block], sem.at[0]))
    for copy in copies:
        copy.start()
    pltpu.make_async_copy(grad_vmem, grad_hbm, sem.at[0]).wait()
    copies[0].wait()


def fused(grad_out, saved_input, keep_bits, gain):
    n_ba, n_aa = lax.axis_size("ba"), lax.axis_size("aa")
    width = grad_out.shape[1]
    rows, depth = saved_input.shape
    n_direct, n_diagonal = len(steps_with(n_ba, 1)), len(steps_with(n_ba, 2))
    f32 = jnp.float32
    grad_in, share = pl.pallas_call(
        functools.partial(kernel, n_ba, n_aa),
        out_shape=(
            pltpu.VMEM((rows, depth), jnp.bfloat16),
            pltpu.VMEM((1, width), f32),
        ),
        in_specs=[pl.BlockSpec(memory_space=pl.ANY)] * 4,
        out_specs=(pl.BlockSpec(memory_space=pltpu.VMEM), pl.BlockSpec(memory_space=pltpu.VMEM)),
        scratch_shapes=[
            pltpu.VMEM((n_ba, rows, width), jnp.bfloat16),
            pltpu.VMEM((n_ba, rows, width), jnp.bfloat16),
            pltpu.VMEM((rows, depth), jnp.bfloat16),
            pltpu.VMEM(keep_bits.shape, jnp.int32),
            pltpu.VMEM((1, depth), f32),
            pltpu.VMEM((rows, depth), f32),
            pltpu.VMEM((rows, depth), f32),
            pltpu.VMEM((rows, LANES), f32),
            pltpu.VMEM((rows, LANES), f32),
            pltpu.VMEM((n_ba, 8, width), f32),
            pltpu.VMEM((n_ba, 1, width), f32),
            pltpu.VMEM((2, 1, width), f32),
            pltpu.VMEM((n_aa * (n_direct + n_diagonal + 1), 1, width), f32),
            pltpu.SemaphoreType.DMA,
            pltpu.SemaphoreType.DMA,
            pltpu.SemaphoreType.DMA,
            pltpu.SemaphoreType.DMA,
            pltpu.SemaphoreType.DMA((2,)),
            pltpu.SemaphoreType.DMA((2,)),
            pltpu.SemaphoreType.DMA,
            pltpu.SemaphoreType.DMA,
            pltpu.SemaphoreType.DMA,
            pltpu.SemaphoreType.DMA,
            pltpu.SemaphoreType.REGULAR,
            pltpu.SemaphoreType.REGULAR((n_aa - 1,)),
            pltpu.VMEM((2, 3, 2, 2, RELAY_ROWS, width), jnp.bfloat16),
            pltpu.SemaphoreType.DMA((2,)),
            pltpu.SemaphoreType.DMA((2,)),
            pltpu.SemaphoreType.DMA((2,)),
        ],
        compiler_params=pltpu.CompilerParams(collective_id=0, has_side_effects=True),
        name="regroup_backward",
    )(grad_out, saved_input, keep_bits, gain.reshape(1, depth))
    grad_in, share = pl.pallas_call(
        store,
        out_shape=(
            jax.ShapeDtypeStruct((rows, depth), jnp.bfloat16),
            jax.ShapeDtypeStruct((1, width), f32),
        ),
        in_specs=[pl.BlockSpec(memory_space=pltpu.VMEM)] * 2,
        out_specs=[pl.BlockSpec(memory_space=pl.ANY)] * 2,
        scratch_shapes=[pltpu.SemaphoreType.DMA((2,))],
        name="store_results",
    )(*(pltpu.with_memory_space_constraint(x, pltpu.VMEM) for x in (grad_in, share)))
    return (grad_in, share.reshape(width))


def per_device(grad_out, saved_input, keep_bits, gain):
    fits = grad_out.shape[1] % LANES == 0 and saved_input.shape[0] % CHUNK_ROWS == 0
    fits = fits and keep_bits.shape[1] == LANES
    n_ba = lax.axis_size("ba")
    fits = fits and n_ba & (n_ba - 1) == 0 and hops(n_ba - 1) == 2 and lax.axis_size("aa") > 1
    body = fused if fits else plain
    return body(grad_out, saved_input, keep_bits, gain)


def solution(mesh):
    placed = (P("aa", "ba"), P(("aa", "ba"), None), P(("aa", "ba"), None), P())
    return jax.shard_map(
        per_device,
        mesh=mesh,
        in_specs=placed,
        out_specs=(P(("aa", "ba"), None), P("ba")),
        check_vma=False,
    )
```

```python
import functools
import math

import jax
import jax.numpy as jnp
from jax import lax
from jax.experimental import pallas as pl
from jax.experimental.pallas import tpu as pltpu
from jax.sharding import PartitionSpec as P

KEEP_RATE = 0.9
EPSILON = 1e-06
LANES = 128
CHUNK_ROWS = 64
STORES = 4
FIRST_ROWS = 64
EARLY_ROWS = 48
RELAY_ROWS = 16
RELAYED = ((2, 2), (1, 1), (1, 1))
MESH = pl.DeviceIdType.MESH


def unpack_bits(words):
    shifts = jnp.arange(32, dtype=jnp.int32)
    bits = jnp.right_shift(words[:, :, None], shifts[None, None, :]) & 1
    return bits.reshape(words.shape[0], words.shape[1] * 32).astype(jnp.float32)


def rows_backward(grad_rows, input_rows, word_rows, gain):
    keep = unpack_bits(word_rows)
    dropped = input_rows.astype(jnp.float32) * keep * (1.0 / KEEP_RATE)
    inverse = lax.rsqrt(jnp.mean(dropped * dropped, axis=-1, keepdims=True) + EPSILON)
    normed = dropped * inverse
    grads = grad_rows.astype(jnp.float32)
    scaled = gain[None, :] * grads
    centre = jnp.mean(scaled * normed, axis=-1, keepdims=True)
    grad_in = (inverse * (scaled - normed * centre) * keep * (1.0 / KEEP_RATE)).astype(jnp.bfloat16)
    partial_sum = jnp.sum(grads * normed, axis=0)
    return (grad_in, partial_sum)


def plain(grad_out, saved_input, keep_bits, gain):
    groups = lax.axis_size("ba")
    rows = grad_out.shape[0] // groups
    pieces = grad_out.reshape(groups, rows, grad_out.shape[1])
    arrived = lax.all_to_all(pieces, "ba", split_axis=0, concat_axis=2, tiled=True)
    grad_rows = arrived.reshape(rows, arrived.shape[2])
    grad_in, partial_sum = rows_backward(grad_rows, saved_input, keep_bits, gain)
    total_tokens = rows * groups * lax.axis_size("aa")
    owned = lax.psum_scatter(partial_sum, "ba", scatter_dimension=0, tiled=True)
    share = lax.psum(owned, "aa")
    gain_grad = share * (1.0 / math.sqrt(total_tokens))
    return (grad_in, gain_grad)


def hops(step):
    return (step >> 1).bit_count()


def steps_with(n_ba, count):
    return sorted((step for step in range(n_ba) if hops(step) == count), key=lambda step: (step % 2, step))


def kernel(n_ba, n_aa, grad_hbm, input_hbm, bits_hbm, gain_hbm, out_ref, share_ref,
           staged, arrived, held, words, gain_ref, normed, masked_gain, outer, totals, sums,
           parts, slices, tails, stage_sem, load_sem, send_sem, small_send, early_recv,
           last_recv, diagonal_recv, sibling_recv, part_recv, tail_recv, ready, flood,
           relayed, relay_recv, relay_send, corner_recv):
    ba, aa = lax.axis_index("ba"), lax.axis_index("aa")
    rows, width = arrived.shape[1], arrived.shape[2]
    depth = n_ba * width
    chunks = rows // CHUNK_ROWS
    tiles = width // LANES
    direct, diagonal = steps_with(n_ba, 1), steps_with(n_ba, 2)
    n_direct, n_diagonal = len(direct), len(diagonal)
    half = n_direct // 2
    per_plane = n_direct + n_diagonal + 1
    order = [0, 1] + direct + diagonal
    slot = {step: place for place, step in enumerate(order)}
    swap = lax.rem(ba // (2 * direct[0]), 2)
    arrivals = [
        (side + offset, 2 + (half if side else 0) + index)
        for offset, index in ((2 + 2 * swap, swap), (4 - 2 * swap, 1 - swap))
        for side in range(2)
    ]
    groups = (arrivals[:half], arrivals[half:])
    early = (0, EARLY_ROWS)
    first_chip = ba < 2
    beside = (ba ^ groups[0][0][0]) < 2
    never = ba < 0

    def kinds(plane, near_first):
        top = plane == n_aa - 1
        second = plane == n_aa - 2 if n_aa > 3 else never
        both = jnp.logical_and
        return (both(top, near_first), both(second, near_first), both(top, jnp.logical_not(near_first)))

    mirror = n_aa - 1 - aa
    odd = lax.rem(ba, 2) == 1
    sends = kinds(aa, first_chip)
    fed = (kinds(aa, beside), kinds(aa, never))
    relays = tuple(
        tuple(jnp.logical_and(flag, odd) for flag in kinds(mirror, near)) for near in (beside, never)
    )

    def either(flags):
        return jnp.logical_or(jnp.logical_or(flags[0], flags[1]), flags[2])

    def last(count):
        return (EARLY_ROWS, rows - EARLY_ROWS - count * RELAY_ROWS)

    def relay_block(index, count=1):
        return pl.ds(rows - (index + count) * RELAY_ROWS, count * RELAY_ROWS)

    def for_kind(flags, action):
        for blocks, flag in zip(RELAYED, flags):
            pl.when(flag)(functools.partial(action, blocks))
        pl.when(jnp.logical_not(either(flags)))(functools.partial(action, (0, 0)))

    def for_core(blocks, action):
        if blocks[0] == blocks[1]:
            action(blocks[0])
        else:
            pl.when(odd)(functools.partial(action, blocks[1]))
            pl.when(jnp.logical_not(odd))(functools.partial(action, blocks[0]))

    def remote_copy(source, target, send, recv, device):
        return pltpu.make_async_remote_copy(
            src_ref=source, dst_ref=target, send_sem=send, recv_sem=recv,
            device_id=device, device_id_type=MESH,
        )

    def column(step):
        return lax.rem(aa + step, n_aa)

    def rows_of(chunk):
        start = chunk * CHUNK_ROWS
        if not isinstance(start, int):
            start = pl.multiple_of(start, CHUNK_ROWS)
        return pl.ds(start, CHUNK_ROWS)

    def stage(step, semaphore):
        first = pl.ds(pl.multiple_of((ba ^ step) * rows, CHUNK_ROWS), rows)
        target = staged.at[slot[step]] if step else arrived.at[0]
        return pltpu.make_async_copy(grad_hbm.at[first], target, semaphore)

    def piece(step, recv, block=None, place=None):
        place = slot[step] if place is None else place
        at = (place, pl.ds(*block)) if block else (place,)
        return remote_copy(staged.at[at], arrived.at[at], send_sem, recv, {"ba": ba ^ step})

    def axis_of(step):
        return 1 if step >= 2 * direct[0] else 0

    def early_piece(step):
        return piece(step, early_recv.at[axis_of(step)], early)

    def last_piece(step, block):
        return piece(step, last_recv.at[axis_of(step)], block)

    def to_relay(step, index):
        target = ba ^ step
        parity = lax.rem(target, 2)
        swapped = lax.rem(target // (2 * direct[0]), 2)
        group = 1 - swapped if axis_of(step) else swapped
        return remote_copy(
            staged.at[slot[step], relay_block(index)], relayed.at[group, index, parity, step % 2],
            send_sem, relay_recv, {"aa": mirror, "ba": target + 1 - parity},
        )

    def from_relay(group, index, parity, cross):
        return remote_copy(
            relayed.at[group, index, parity, cross], arrived.at[groups[group][cross][1], relay_block(index)],
            relay_send, corner_recv.at[group], {"aa": mirror, "ba": ba - 1 + parity},
        )

    def relay_all(count):
        blocks = relayed.at[0, pl.ds(0, count)] if count < 3 else relayed.at[0]
        return remote_copy(blocks, blocks, relay_send, relay_recv, {"ba": ba ^ 1})

    def landed(recv, *at):
        return remote_copy(staged.at[at], arrived.at[at], send_sem, recv, {"ba": ba ^ 1})

    def part():
        return remote_copy(parts.at[1], slices.at[1], small_send, part_recv, {"ba": ba ^ 1})

    def share(step):
        mine = tails.at[aa * per_plane]
        return remote_copy(mine, mine, small_send, tail_recv, {"aa": column(step)})

    def late(target, step, place):
        return remote_copy(
            parts.at[place], tails.at[aa * per_plane + place - 1], small_send, tail_recv,
            {"aa": target, "ba": ba ^ step},
        )

    def greet_column(semaphore):
        @pl.when(aa > 0)
        def _():
            pl.semaphore_signal(semaphore, inc=1, device_id={"aa": aa - 1}, device_id_type=MESH)

        @pl.when(aa < n_aa - 1)
        def _():
            pl.semaphore_signal(semaphore, inc=1, device_id={"aa": aa + 1}, device_id_type=MESH)

    column_peers = (aa > 0).astype(jnp.int32) + (aa < n_aa - 1).astype(jnp.int32)

    barrier = pltpu.get_barrier_semaphore()
    for step in direct + [1]:
        pl.semaphore_signal(barrier, inc=1, device_id={"ba": ba ^ step}, device_id_type=MESH)
    greet_column(barrier)

    for group in range(2):
        @pl.when(either(relays[group]))
        def _(group=group):
            for step, _ in groups[group]:
                pl.semaphore_signal(
                    barrier, inc=1, device_id={"aa": mirror, "ba": ba ^ step}, device_id_type=MESH)

    for step in order[1:]:
        stage(step, stage_sem).start()
    loads = [
        pltpu.make_async_copy(bits_hbm, words, load_sem),
        pltpu.make_async_copy(gain_hbm, gain_ref, load_sem),
        pltpu.make_async_copy(input_hbm, held, load_sem),
        stage(0, load_sem),
    ]
    for load in loads:
        load.start()
    with jax.named_scope("w_barrier"):
        pl.semaphore_wait(barrier, n_direct + 1 + column_peers + half * either(sends).astype(jnp.int32))
    pl.semaphore_signal(ready, inc=1, device_id={"ba": ba ^ direct[0]}, device_id_type=MESH)
    with jax.named_scope("w_stage"):
        everything = pl.ds(1, n_ba - 1)
        pltpu.make_async_copy(staged.at[everything], staged.at[everything], stage_sem).wait()
    for step in direct:
        early_piece(step).start()

    def start_relays(blocks):
        def start(count):
            for index in range(count):
                for step in direct:
                    to_relay(step, index).start()

        for_core(blocks, start)

    for_kind(sends, start_relays)

    piece(1, sibling_recv).start()
    with jax.named_scope("w_ready"):
        pl.semaphore_wait(ready, 1)
    greet_column(flood.at[0])
    for step in diagonal:
        piece(step, diagonal_recv).start()

    def start_last(blocks):
        def start(count):
            for step in direct:
                last_piece(step, last(count)).start()

        for_core(blocks, start)

    for_kind(sends, start_last)
    with jax.named_scope("w_load"):
        for load in loads:
            load.wait()

    lane = lax.broadcasted_iota(jnp.int32, (CHUNK_ROWS, LANES), 1)
    word_of = lane // 32
    flag = jnp.left_shift(jnp.int32(1), lane % 32)

    def span(source, tile):
        return pl.ds(pl.multiple_of(source * width + tile * LANES, LANES), LANES)

    def prepare(chunk, carry):
        block = rows_of(chunk)

        def drop(source, squares):
            row_words = words[block, :]
            for tile in range(tiles):
                at = span(source, tile)
                index = word_of + (source * tiles + tile) * (LANES // 32)
                spread = jnp.take_along_axis(row_words, index, axis=1, mode="promise_in_bounds")
                kept = (spread & flag) != 0
                dropped = jnp.where(kept, held[block, at].astype(jnp.float32), 0.0) * (1.0 / KEEP_RATE)
                normed[block, at] = dropped
                masked_gain[block, at] = jnp.where(kept, gain_ref[:, at], 0.0)
                squares = squares + dropped * dropped
            return squares

        squares = lax.fori_loop(0, n_ba, drop, jnp.zeros((CHUNK_ROWS, LANES), jnp.float32))
        mean = jnp.sum(squares, axis=1, keepdims=True) * (1.0 / depth)
        inverse = lax.rsqrt(mean + EPSILON)
        outer[block, :] = jnp.broadcast_to(inverse * (1.0 / KEEP_RATE), (CHUNK_ROWS, LANES))

        def scale(source, none):
            for tile in range(tiles):
                at = span(source, tile)
                normed[block, at] = normed[block, at] * inverse
            return none

        lax.fori_loop(0, n_ba, scale, 0)
        return carry

    with jax.named_scope("prepare"):
        lax.fori_loop(0, chunks, prepare, 0)
    sums[...] = jnp.zeros_like(sums)
    totals[...] = jnp.zeros_like(totals)

    def first(step, place, start, size):
        source = ba ^ step

        def some(block, count):
            total = totals[block, :]
            for tile in range(tiles):
                at = span(source, tile)
                here = slice(tile * LANES, (tile + 1) * LANES)
                grads = arrived[place, block, here].astype(jnp.float32)
                product = grads * normed[block, at]
                total = total + product * gain_ref[:, at]
                sums[place, :, here] += jnp.sum(product.reshape(count // 8, 8, LANES), axis=0)
            totals[block, :] = total

        if size % FIRST_ROWS:
            some(pl.ds(start, size), size)
        else:
            def more(index, none):
                some(pl.ds(pl.multiple_of(start + index * FIRST_ROWS, RELAY_ROWS), FIRST_ROWS), FIRST_ROWS)
                return none

            lax.fori_loop(0, size // FIRST_ROWS, more, 0)

    def finish(chunk, none):
        block = rows_of(chunk)
        factor = outer[block, :]
        centre = jnp.sum(totals[block, :], axis=1, keepdims=True) * (1.0 / depth)

        for step in order:
            for tile in range(tiles):
                at = span(ba ^ step, tile)
                grads = arrived[slot[step], block, tile * LANES:(tile + 1) * LANES].astype(jnp.float32)
                value = factor * (masked_gain[block, at] * grads - normed[block, at] * centre)
                out_ref[block, at] = value.astype(jnp.bfloat16)
        return none

    def fold(place):
        return jnp.sum(sums[place], axis=0, keepdims=True)

    def send_late(step, place):
        parts[place] = fold(place)
        for target in range(n_aa):
            late(target, step, place).start()

    def meet(turn):
        with jax.named_scope(f"w_flood{turn}"):
            pl.semaphore_wait(flood.at[turn], column_peers)
        if turn < n_aa - 2:
            greet_column(flood.at[turn + 1])

    axes = (swap, 1 - swap)

    def take_early(group):
        with jax.named_scope("w_early"):
            landed(early_recv.at[axes[group]], pl.ds(2, half), pl.ds(*early)).wait_recv()
        for step, place in groups[group]:
            first(step, place, *early)

    first(0, 0, 0, rows)
    slices[0] = fold(0)
    with jax.named_scope("w_sibling"):
        piece(1, sibling_recv).wait_recv()
    first(1, 1, 0, rows)
    parts[1] = fold(1)
    part().start()
    meet(0)

    others_relayed = RELAYED[2]

    def both_groups(kind):
        return (RELAYED[kind], (0, 0) if kind == 1 else others_relayed)

    def relay_total(kind):
        return sum(sum(blocks) for blocks in both_groups(kind)) // 2

    def pass_on(kind):
        with jax.named_scope("w_relay"):
            relay_all(relay_total(kind)).wait_recv()
        for group, blocks in enumerate(both_groups(kind)):
            for parity in range(2):
                for cross in range(2):
                    for index in range(blocks[parity ^ cross]):
                        from_relay(group, index, parity, cross).start()

    for kind, flag in enumerate(relays[0]):
        pl.when(flag)(functools.partial(pass_on, kind))
    for turn in range(1, n_aa - 1):
        meet(turn)
    with jax.named_scope("w_part"):
        part().wait_recv()
    tails[aa * per_plane] = slices[0] + slices[1]
    for step in range(1, n_aa):
        share(step).start()
    def take_diagonal():
        with jax.named_scope("w_diag"):
            landed(diagonal_recv, pl.ds(2 + n_direct, n_diagonal)).wait_recv()
        for step in diagonal:
            first(step, slot[step], 0, rows)
            send_late(step, slot[step])

    def land_group(group, blocks):
        count = sum(blocks) // 2
        if count:
            with jax.named_scope("w_corner"):
                landed(corner_recv.at[group], pl.ds(2, half), relay_block(0, count)).wait_recv()
        with jax.named_scope("w_last"):
            landed(last_recv.at[axes[group]], pl.ds(2, half), pl.ds(*last(count))).wait_recv()

    def take_group(group):
        for_kind(fed[group], functools.partial(land_group, group))
        for turn in range(2):
            cross = lax.rem(ba + turn, 2)
            step, place = groups[group][0][0] + cross, groups[group][0][1] + half * cross
            first(step, place, EARLY_ROWS, rows - EARLY_ROWS)
            send_late(step, place)

    pl.when(jnp.logical_not(beside))(take_diagonal)
    take_early(0)
    take_group(0)
    pl.when(beside)(take_diagonal)
    take_early(1)
    take_group(1)
    with jax.named_scope("finish"):
        lax.fori_loop(0, chunks, finish, 0)
    with jax.named_scope("w_tail"):
        others = tails.at[pl.ds(0, n_aa * per_plane - 1)]
        remote_copy(others, others, small_send, tail_recv, {"ba": ba ^ 1}).wait_recv()
    with jax.named_scope("final_sum"):
        total = jnp.sum(tails[...], axis=0)
        share_ref[...] = total * (1.0 / math.sqrt(rows * n_ba * n_aa))
    with jax.named_scope("w_last_sends"):
        landed(sibling_recv, everything).wait_send()

        for kind, flag in enumerate(relays[0]):
            @pl.when(flag)
            def _(kind=kind):
                relay_all(relay_total(kind)).wait_send()

        remote_copy(tails, tails, small_send, tail_recv, {"ba": ba ^ 1}).wait_send()


def store(grad_vmem, share_vmem, grad_hbm, share_hbm, sem):
    rows = grad_vmem.shape[0] // STORES
    copies = [pltpu.make_async_copy(share_vmem, share_hbm, sem.at[1])]
    for index in range(STORES):
        block = pl.ds(index * rows, rows)
        copies.append(pltpu.make_async_copy(grad_vmem.at[block], grad_hbm.at[block], sem.at[0]))
    for copy in copies:
        copy.start()
    pltpu.make_async_copy(grad_vmem, grad_hbm, sem.at[0]).wait()
    copies[0].wait()


def fused(grad_out, saved_input, keep_bits, gain):
    n_ba, n_aa = lax.axis_size("ba"), lax.axis_size("aa")
    width = grad_out.shape[1]
    rows, depth = saved_input.shape
    n_direct, n_diagonal = len(steps_with(n_ba, 1)), len(steps_with(n_ba, 2))
    f32 = jnp.float32
    grad_in, share = pl.pallas_call(
        functools.partial(kernel, n_ba, n_aa),
        out_shape=(
            pltpu.VMEM((rows, depth), jnp.bfloat16),
            pltpu.VMEM((1, width), f32),
        ),
        in_specs=[pl.BlockSpec(memory_space=pl.ANY)] * 4,
        out_specs=(pl.BlockSpec(memory_space=pltpu.VMEM), pl.BlockSpec(memory_space=pltpu.VMEM)),
        scratch_shapes=[
            pltpu.VMEM((n_ba, rows, width), jnp.bfloat16),
            pltpu.VMEM((n_ba, rows, width), jnp.bfloat16),
            pltpu.VMEM((rows, depth), jnp.bfloat16),
            pltpu.VMEM(keep_bits.shape, jnp.int32),
            pltpu.VMEM((1, depth), f32),
            pltpu.VMEM((rows, depth), f32),
            pltpu.VMEM((rows, depth), f32),
            pltpu.VMEM((rows, LANES), f32),
            pltpu.VMEM((rows, LANES), f32),
            pltpu.VMEM((n_ba, 8, width), f32),
            pltpu.VMEM((n_ba, 1, width), f32),
            pltpu.VMEM((2, 1, width), f32),
            pltpu.VMEM((n_aa * (n_direct + n_diagonal + 1), 1, width), f32),
            pltpu.SemaphoreType.DMA,
            pltpu.SemaphoreType.DMA,
            pltpu.SemaphoreType.DMA,
            pltpu.SemaphoreType.DMA,
            pltpu.SemaphoreType.DMA((2,)),
            pltpu.SemaphoreType.DMA((2,)),
            pltpu.SemaphoreType.DMA,
            pltpu.SemaphoreType.DMA,
            pltpu.SemaphoreType.DMA,
            pltpu.SemaphoreType.DMA,
            pltpu.SemaphoreType.REGULAR,
            pltpu.SemaphoreType.REGULAR((n_aa - 1,)),
            pltpu.VMEM((2, 3, 2, 2, RELAY_ROWS, width), jnp.bfloat16),
            pltpu.SemaphoreType.DMA,
            pltpu.SemaphoreType.DMA,
            pltpu.SemaphoreType.DMA((2,)),
        ],
        compiler_params=pltpu.CompilerParams(collective_id=0, has_side_effects=True),
        name="regroup_backward",
    )(grad_out, saved_input, keep_bits, gain.reshape(1, depth))
    grad_in, share = pl.pallas_call(
        store,
        out_shape=(
            jax.ShapeDtypeStruct((rows, depth), jnp.bfloat16),
            jax.ShapeDtypeStruct((1, width), f32),
        ),
        in_specs=[pl.BlockSpec(memory_space=pltpu.VMEM)] * 2,
        out_specs=[pl.BlockSpec(memory_space=pl.ANY)] * 2,
        scratch_shapes=[pltpu.SemaphoreType.DMA((2,))],
        name="store_results",
    )(*(pltpu.with_memory_space_constraint(x, pltpu.VMEM) for x in (grad_in, share)))
    return (grad_in, share.reshape(width))


def per_device(grad_out, saved_input, keep_bits, gain):
    fits = grad_out.shape[1] % LANES == 0 and saved_input.shape[0] % CHUNK_ROWS == 0
    fits = fits and keep_bits.shape[1] == LANES
    n_ba = lax.axis_size("ba")
    fits = fits and n_ba & (n_ba - 1) == 0 and hops(n_ba - 1) == 2 and lax.axis_size("aa") > 1
    body = fused if fits else plain
    return body(grad_out, saved_input, keep_bits, gain)


def solution(mesh):
    placed = (P("aa", "ba"), P(("aa", "ba"), None), P(("aa", "ba"), None), P())
    return jax.shard_map(
        per_device,
        mesh=mesh,
        in_specs=placed,
        out_specs=(P(("aa", "ba"), None), P("ba")),
        check_vma=False,
    )
```
